32 devices in a mesh: dp: 8 (over z, y), ep: 4 (over x, core).
Axes of the slice: x: 2, y: 2, z: 4, core: 2. Of those that a mesh axis runs over, the one named last changes fastest.
Arguments:
- w_gate: bfloat16 [1, 16, 2048, 1024], P(None, 'ep')
- w_up: bfloat16 [1, 16, 2048, 1024], P(None, 'ep')
- w_down: bfloat16 [1, 16, 1024, 2048], P(None, 'ep')
- place: int32 [1, 64], replicated
Outputs:
- output 1: bfloat16 [1, 64, 2048, 2048], P(None, ('dp', 'ep'))
- output 2: bfloat16 [1, 64, 1024, 2048], P(None, ('dp', 'ep'))
All inputs are finite; a program needn't handle non-finite values.
Results may differ from the reference program's by a relative error of at most 0.001.
Values are sent between devices in bfloat16 or wider.
A program may use at most 1 GiB of HBM per device.

```python
import jax
import jax.numpy as jnp
import numpy as np

D = 2048
F = 1024
E = 16
L = 1
SLOTS = 2
DP = 8
EP = 4


def _slot_shard():
    n = np.arange(DP * EP)[:, None]
    j = np.arange(SLOTS)[None, :]
    a, g = n // EP, n % EP
    h = np.where(j < ((a + 1) * SLOTS) // DP, (2 * a - g) % EP, (g + j + 1) % EP)
    return h.reshape(-1)


def _draw_place(key):
    shard = E // EP
    width = DP * SLOTS

    def one(k):
        k1, k2, k3 = jax.random.split(k, 3)
        base = jax.random.permutation(k1, shard)
        extra = jax.random.randint(k2, (width - shard,), 0, shard)
        return jax.random.permutation(k3, jnp.concatenate([base, extra]))

    local = jax.vmap(one)(jax.random.split(key, L * EP)).reshape(L, EP, width)
    glob = (local + (jnp.arange(EP) * shard)[None, :, None]).reshape(L, EP * width)
    order = np.argsort(_slot_shard(), kind="stable")
    out = jnp.zeros((L, EP * width), jnp.int32).at[:, order].set(glob.astype(jnp.int32))
    return out


def setup_inputs(seed: int = 0) -> dict:
    kg, ku, kd, kp = jax.random.split(jax.random.PRNGKey(seed), 4)
    w_gate = jax.random.normal(kg, (L, E, D, F), jnp.float32).astype(jnp.bfloat16)
    w_up = jax.random.normal(ku, (L, E, D, F), jnp.float32).astype(jnp.bfloat16)
    w_down = jax.random.normal(kd, (L, E, F, D), jnp.float32).astype(jnp.bfloat16)
    return {"w_gate": w_gate, "w_up": w_up, "w_down": w_down, "place": _draw_place(kp)}


def reference(w_gate, w_up, w_down, place):
    take = jax.vmap(lambda w, i: w[i])
    w13 = jnp.concatenate([take(w_gate, place), take(w_up, place)], axis=-1)
    return w13, take(w_down, place)
```

```python
import functools

import jax
import jax.numpy as jnp
from jax import lax
from jax.experimental import pallas as pl
from jax.experimental.pallas import tpu as pltpu
from jax.sharding import PartitionSpec as P

UNITS = 32
RING = 4
ORING = 4
DSTAGE = 32
HUB = ((3, 2, 8, 8, 4, 4, 1, 2), (0, 0, 0, 0, 8, 8, 8, 8))
SERVE = (
    ((3, 3, 3, 3, 2, 2, 0, 0), (2, 2, 2, 2, 1, 2, 0, 2), (8, 8, 8, 8, 8, 8, 8, 6), (8, 8, 8, 8, 8, 8, 1, 8),
     (4, 0, 4, 4, 4, 4, 4, 4), (0, 4, 3, 4, 4, 4, 4, 4), (0, 0, 0, 0, 1, 1, 1, 1), (0, 0, 0, 0, 2, 2, 2, 2)),
    ((0, 0, 0, 0, 0, 0, 0, 0), (0, 0, 0, 0, 0, 0, 0, 0), (0, 0, 0, 0, 0, 0, 0, 0), (0, 0, 0, 0, 0, 0, 0, 0),
     (8, 0, 8, 4, 8, 8, 8, 0), (0, 4, 8, 8, 8, 8, 8, 0), (0, 0, 6, 0, 8, 8, 8, 0), (0, 0, 0, 8, 8, 8, 8, 0)),
)
KIND = []
for _a in range(8):
    _row = []
    for _c in range(2):
        for _j in range(2):
            _g = _c + 2
            _h = (2 * _a - _g) % 4 if _j < ((_a + 1) * 2) // 8 else (_g + _j + 1) % 4
            _row.append(_h if _h < 2 else (3 if _h == _g else 2))
    KIND.append(_row)
SLOTS = tuple(tuple((a, s // 2, s % 2) for a in range(8) for s in range(4) if KIND[a][s] == c) for c in range(2))
MAXS = max(len(s) for s in SLOTS)
FIRST = tuple(tuple(sum(HUB[c][:v]) for v in range(8)) for c in range(2))


def _direct(c, u):
    if not any(s[0] == u for s in SLOTS[c]):
        return []
    out = []
    for v in range(8):
        lo, hi = FIRST[c][v] + SERVE[c][v][u], FIRST[c][v] + HUB[c][v]
        if lo == hi:
            continue
        if out and out[-1][1] == lo:
            out[-1][1] = hi
        else:
            out.append([lo, hi])
    return out


DIRECT = tuple(tuple(_direct(c, u) for u in range(8)) for c in range(2))
NDIR = tuple(tuple(sum(hi - lo for lo, hi in r) for r in DIRECT[c]) for c in range(2))


def _pick(table, i):
    r = jnp.int32(table[0])
    for k in range(1, len(table)):
        if table[k] != table[0]:
            r = jnp.where(i == k, jnp.int32(table[k]), r)
    return r


def _remote(place, wg, wu, wd, r13, r2, raw_g, raw_u, raw_d, dw_g, dw_u, dw_d, wk13, wk2, hs_g, hs_u, hs_d,
            ds_g, ds_u, ds_d, os_g, os_u, os_d, raw_rx, raw_tx, h_tx, d_tx, o_tx, ld, rx):
    a = lax.axis_index("dp")
    g = lax.axis_index("ep")
    x = g // 2
    core = g % 2
    w, raw, dw = (wg, wu, wd), (raw_g, raw_u, raw_d), (dw_g, dw_u, dw_d)
    hs, ds, os_, wk = (hs_g, hs_u, hs_d), (ds_g, ds_u, ds_d), (os_g, os_u, os_d), (wk13, wk13, wk2)
    nexp, f = wg.shape[1], wg.shape[3]
    rows = tuple(r.shape[2] for r in raw)

    def expert(s, h):
        return jnp.clip(place[0, s] - h * nexp, 0, nexp - 1)

    def unit(t, k):
        return pl.ds(pl.multiple_of(k * rows[t], rows[t]), rows[t])

    def landing(t, j, k):
        if t == 2:
            return r2.at[j, unit(t, k)]
        return r13.at[j, unit(t, k), pl.ds(t * f, f)]

    def send(t, src, j, k, tx, ua, uep):
        return pltpu.make_async_remote_copy(
            src_ref=src, dst_ref=landing(t, j, k), send_sem=tx, recv_sem=rx.at[j, t],
            device_id={"dp": ua, "ep": uep}, device_id_type=pl.DeviceIdType.MESH)

    for c in range(2):

        @pl.when(core == c)
        def _(c=c):
            width = _pick(HUB[c], a)
            first = _pick(FIRST[c], a)
            slots = SLOTS[c]
            served = [_pick([SERVE[c][v][s[0]] for v in range(8)], a) for s in slots]

            def raw_copy(i, t):
                return pltpu.make_async_remote_copy(
                    src_ref=w[t].at[0, :, unit(t, first + i)], dst_ref=raw[t].at[i],
                    send_sem=raw_tx.at[t, i], recv_sem=raw_rx.at[t, i],
                    device_id={"dp": a, "ep": 2 * (1 - x) + c}, device_id_type=pl.DeviceIdType.MESH)

            def raw_start(i, _):
                for t in range(3):
                    raw_copy(i, t).start()
                return _

            lax.fori_loop(0, width, raw_start, 0)

            dslots = [[(s[1], s[2]) for s in slots if s[0] == u] if NDIR[c][u] else [] for u in range(8)]
            per = max(len(s) for s in dslots)
            ndir = _pick(NDIR[c], a)
            nranges = max(len(r) for r in DIRECT[c])
            starts, steps = [], []
            base = _pick([r[0][0] if r else 0 for r in DIRECT[c]], a)
            for q in range(1, nranges):
                starts.append(_pick([sum(hi - lo for lo, hi in r[:q]) if len(r) > q else 999 for r in DIRECT[c]], a))
                steps.append(_pick([r[q][0] - r[q - 1][1] if len(r) > q else 0 for r in DIRECT[c]], a))

            nown = _pick([UNITS if 2 in KIND[u][:2] else 0 for u in range(8)], a) if c == 1 else jnp.int32(0)
            njobs = ndir + nown

            def dunit(n):
                k = base + n
                for st, sp in zip(starts, steps):
                    k = k + jnp.where(n >= st, sp, 0)
                if c == 1:
                    k = jnp.where(n >= ndir, n - ndir, k)
                return k

            def load(n, t):
                return pltpu.make_async_copy(w[t].at[0, :, unit(t, dunit(n))], dw[t].at[n % 2], ld.at[t, n % 2])

            dtab = []
            for q in range(per):
                dtab.append((_pick([len(s) > q for s in dslots], a),
                             _pick([s[q][0] if len(s) > q else 0 for s in dslots], a),
                             _pick([s[q][1] if len(s) > q else 0 for s in dslots], a)))

            def dsend(n, t, q):
                _, uc, j = dtab[q]
                return send(t, ds[t].at[n * per + q], j, dunit(n), d_tx.at[t, n * per + q], a, 2 * (1 - x) + uc)

            def osend(n, t):
                return send(t, os_[t].at[n % ORING], 0, n, o_tx.at[t, n % ORING], a, 2 * x)

            @pl.when(njobs > 0)
            def _():
                for t in range(3):
                    load(0, t).start()

            def direct(n):
                for t in range(3):
                    load(n, t).wait()
                    wk[t][...] = dw[t][n % 2]

                    @pl.when(n + 1 < njobs)
                    def _():
                        load(n + 1, t).start()

                    @pl.when(n < ndir)
                    def _():
                        for q in range(per):
                            on, uc, j = dtab[q]

                            @pl.when(on == 1)
                            def _():
                                e = expert((a * 4 + 2 * (1 - x) + uc) * 2 + j, 2 * x + c)
                                ds[t][n * per + q] = wk[t][e]

                        for q in range(per):

                            @pl.when(dtab[q][0] == 1)
                            def _():
                                dsend(n, t, q).start()

                    if c == 1:

                        @pl.when(n >= ndir)
                        def _():
                            m = n - ndir

                            @pl.when(m >= ORING)
                            def _():
                                osend(m - ORING, t).wait_send()

                            e = expert((a * 4 + 2 * x) * 2, 2 * x + c)
                            os_[t][m % ORING] = wk[t][e]
                            osend(m, t).start()

            def hub_copy(i, t, q):
                ua, uc, j = slots[q]
                src, tx = hs[t].at[i % RING, q], h_tx.at[t, i % RING, q]
                there = send(t, src, j, first + i, tx, ua, 2 * x + uc)
                here = pltpu.make_async_copy(src, landing(t, j, first + i), tx) if uc == c else None
                return there, here

            def hub_do(i, t, q, start):
                ua, uc, _ = slots[q]
                there, here = hub_copy(i, t, q)
                if here is None:
                    there.start() if start else there.wait_send()
                    return

                @pl.when(a == ua)
                def _():
                    here.start() if start else here.wait()

                @pl.when(a != ua)
                def _():
                    there.start() if start else there.wait_send()

            def hub_free(i, t):
                for q in range(len(slots)):

                    @pl.when(i < served[q])
                    def _():
                        hub_do(i, t, q, False)

            def hub(i):
                for t in range(3):

                    @pl.when(i >= RING)
                    def _():
                        hub_free(i - RING, t)

                    raw_copy(i, t).wait_recv()
                    wk[t][...] = raw[t][i]
                    for q in range(len(slots)):
                        ua, uc, j = slots[q]

                        @pl.when(i < served[q])
                        def _():
                            e = expert((ua * 4 + 2 * x + uc) * 2 + j, 2 * (1 - x) + c)
                            hs[t][i % RING, q] = wk[t][e]

                    for q in range(len(slots)):

                        @pl.when(i < served[q])
                        def _():
                            hub_do(i, t, q, True)

            def step(i, _):
                @pl.when(i < njobs)
                def _():
                    direct(i)

                @pl.when(i < width)
                def _():
                    hub(i)

                return _

            lax.fori_loop(0, jnp.maximum(width, njobs), lambda i, s: (step(i, s), s)[1], 0)

            def hub_drain(i, s):
                for t in range(3):
                    hub_free(i, t)
                return s

            lax.fori_loop(jnp.maximum(width - RING, 0), width, hub_drain, 0)

            def direct_drain(n, s):
                for t in range(3):
                    for q in range(per):

                        @pl.when(dtab[q][0] == 1)
                        def _():
                            dsend(n, t, q).wait_send()
                return s

            lax.fori_loop(0, ndir, direct_drain, 0)
            if c == 1:

                def own_drain(n, s):
                    for t in range(3):
                        osend(n, t).wait_send()
                    return s

                lax.fori_loop(jnp.maximum(nown - ORING, 0), nown, own_drain, 0)

            def raw_drain(i, s):
                for t in range(3):
                    raw_copy(i, t).wait_send()
                return s

            lax.fori_loop(0, width, raw_drain, 0)

            for u in range(8):

                @pl.when(a == u)
                def _(u=u):
                    for j in range(2):
                        kind = KIND[u][2 * c + j]
                        if kind == 3:
                            continue
                        n = UNITS - (SERVE[c][u][u] if kind == c else 0)
                        for t in range(3):
                            if t == 2:
                                part = r2.at[j, pl.ds(0, n * rows[2])]
                            else:
                                part = r13.at[j, pl.ds(0, n * rows[t]), pl.ds(t * f, f)]
                            pltpu.make_async_copy(part, part, rx.at[j, t]).wait()


def _local(nblk, place, wg, wu, wd, r13, r2, o13, o2, buf, lsem, ssem):
    a = lax.axis_index("dp")
    g = lax.axis_index("ep")
    nexp, f = wg.shape[1], wg.shape[3]
    b13 = r13.shape[1] // nblk[0]
    b2 = r2.shape[1] // nblk[1]
    n = 0
    jobs = []
    for j in range(2):
        own = jnp.int32(0)
        for u in range(8):
            for c in range(2):
                if KIND[u][2 * c + j] == 3:
                    own = jnp.where((a == u) & (g % 2 == c), 1, own)
        e = jnp.clip(place[0, (a * 4 + g) * 2 + j] - g * nexp, 0, nexp - 1)
        for b in range(nblk[0] + nblk[1]):
            jobs.append((n, j, b, own, e))
            n += 1
    for n, j, b, own, e in jobs:
        wide = b < nblk[0]
        r = pl.ds(b * b13, b13) if wide else pl.ds((b - nblk[0]) * b2, b2)

        @pl.when(own == 1)
        def _():
            if wide:
                pltpu.make_async_copy(wg.at[0, e, r], buf.at[n, :, pl.ds(0, f)], lsem.at[n]).start()
                pltpu.make_async_copy(wu.at[0, e, r], buf.at[n, :, pl.ds(f, f)], lsem.at[n]).start()
            else:
                pltpu.make_async_copy(wd.at[0, e, r], buf.at[n], lsem.at[n]).start()

        @pl.when(own == 0)
        def _():
            pltpu.make_async_copy((r13 if wide else r2).at[j, r], buf.at[n], lsem.at[n]).start()

    stores = []
    for n, j, b, own, e in jobs:
        wide = b < nblk[0]
        r = pl.ds(b * b13, b13) if wide else pl.ds((b - nblk[0]) * b2, b2)
        pltpu.make_async_copy(buf.at[n], buf.at[n], lsem.at[n]).wait()
        st = pltpu.make_async_copy(buf.at[n], (o13 if wide else o2).at[0, j, r], ssem.at[n])
        st.start()
        stores.append(st)
    for st in stores:
        st.wait()


def solution(mesh):
    anyspec = pl.BlockSpec(memory_space=pl.ANY)
    smem = pl.BlockSpec(memory_space=pltpu.SMEM)

    def body(wg, wu, wd, place):
        _, nexp, d, f = wg.shape
        dt = wg.dtype
        ra, rb = d // UNITS, f // UNITS
        wmax = max(max(h) for h in HUB)
        dma = pltpu.SemaphoreType.DMA

        def three(*lead):
            return [pltpu.VMEM((*lead, ra, f), dt), pltpu.VMEM((*lead, ra, f), dt), pltpu.VMEM((*lead, rb, d), dt)]

        r13, r2 = pl.pallas_call(
            _remote,
            out_shape=(jax.ShapeDtypeStruct((2, d, 2 * f), dt), jax.ShapeDtypeStruct((2, f, d), dt)),
            in_specs=[smem, anyspec, anyspec, anyspec],
            out_specs=(anyspec, anyspec),
            scratch_shapes=[
                *three(wmax, nexp), *three(2, nexp),
                pltpu.VMEM((nexp, ra, f), dt), pltpu.VMEM((nexp, rb, d), dt),
                *three(RING, MAXS), *three(DSTAGE), *three(ORING),
                dma((3, wmax)), dma((3, wmax)), dma((3, RING, MAXS)), dma((3, DSTAGE)), dma((3, ORING)),
                dma((3, 2)), dma((2, 3)),
            ],
            compiler_params=pltpu.CompilerParams(has_side_effects=True, vmem_limit_bytes=62 * 1024 * 1024),
            name="spread",
        )(place, wg, wu, wd)
        nblk = (8, 4)
        nbuf = 2 * sum(nblk)
        return pl.pallas_call(
            functools.partial(_local, nblk),
            out_shape=(jax.ShapeDtypeStruct((1, 2, d, 2 * f), dt), jax.ShapeDtypeStruct((1, 2, f, d), dt)),
            in_specs=[smem, anyspec, anyspec, anyspec, anyspec, anyspec],
            out_specs=(anyspec, anyspec),
            scratch_shapes=[pltpu.VMEM((nbuf, d // nblk[0], 2 * f), dt), dma((nbuf,)), dma((nbuf,))],
            compiler_params=pltpu.CompilerParams(vmem_limit_bytes=48 * 1024 * 1024),
            name="settle",
        )(place, wg, wu, wd, r13, r2)

    spec_in = P(None, "ep", None, None)
    spec_out = P(None, ("dp", "ep"), None, None)
    return jax.shard_map(body, mesh=mesh, in_specs=(spec_in, spec_in, spec_in, P(None, None)),
                         out_specs=(spec_out, spec_out), check_vma=False)
```

```python
import functools

import jax
import jax.numpy as jnp
from jax import lax
from jax.experimental import pallas as pl
from jax.experimental.pallas import tpu as pltpu
from jax.sharding import PartitionSpec as P

SUB = 1
UNITS = 32 * SUB
RING = 6 * SUB
ORING = 4
OWN = 8 * SUB
DSTAGE = 28 * SUB
HUB = ((4, 4, 6, 6, 4, 4, 2, 2), (0, 0, 4, 4, 6, 6, 6, 6))
SERVE = (((4, 4, 4, 4, 0, 0, 0, 0), (4, 4, 4, 4, 0, 4, 0, 0), (6, 6, 6, 6, 6, 4, 6, 4), (6, 6, 6, 6, 6, 6, 2, 6), (3, 0, 4, 3, 4, 4, 4, 4), (0, 3, 3, 4, 4, 4, 4, 4), (0, 0, 2, 0, 2, 2, 2, 2), (0, 0, 0, 2, 2, 2, 2, 2)), ((0, 0, 0, 0, 0, 0, 0, 0), (0, 0, 0, 0, 0, 0, 0, 0), (4, 4, 4, 4, 4, 4, 4, 0), (4, 4, 4, 4, 2, 4, 0, 0), (6, 0, 6, 6, 6, 6, 6, 0), (0, 6, 6, 6, 6, 6, 6, 0), (0, 0, 6, 0, 6, 6, 6, 0), (0, 0, 0, 6, 6, 6, 6, 0)))
HUB = tuple(tuple(w * SUB for w in h) for h in HUB)
SERVE = tuple(tuple(tuple(w * SUB for w in r) for r in h) for h in SERVE)
KIND = []
for _a in range(8):
    _row = []
    for _c in range(2):
        for _j in range(2):
            _g = _c + 2
            _h = (2 * _a - _g) % 4 if _j < ((_a + 1) * 2) // 8 else (_g + _j + 1) % 4
            _row.append(_h if _h < 2 else (3 if _h == _g else 2))
    KIND.append(_row)
SLOTS = tuple(tuple((a, s // 2, s % 2) for a in range(8) for s in range(4) if KIND[a][s] == c) for c in range(2))
MAXS = max(len(s) for s in SLOTS)
FIRST = tuple(tuple(sum(HUB[c][:v]) for v in range(8)) for c in range(2))


def _direct(c, u):
    if not any(s[0] == u for s in SLOTS[c]):
        return []
    out = []
    parts = [(FIRST[c][v] + SERVE[c][v][u], FIRST[c][v] + HUB[c][v]) for v in range(8)]
    for lo, hi in parts + [(sum(HUB[c]), UNITS)]:
        if lo == hi:
            continue
        if out and out[-1][1] == lo:
            out[-1][1] = hi
        else:
            out.append([lo, hi])
    return out


DIRECT = tuple(tuple(_direct(c, u) for u in range(8)) for c in range(2))
NDIR = tuple(tuple(sum(hi - lo for lo, hi in r) for r in DIRECT[c]) for c in range(2))


def _pick(table, i):
    r = jnp.int32(table[0])
    for k in range(1, len(table)):
        if table[k] != table[0]:
            r = jnp.where(i == k, jnp.int32(table[k]), r)
    return r


def _remote(place, wg, wu, wd, r13, r2, raw_g, raw_u, raw_d, dw_g, dw_u, dw_d, wk13, wk2, hs_g, hs_u, hs_d,
            ds_g, ds_u, ds_d, os_g, os_u, os_d, raw_rx, raw_tx, h_tx, d_tx, o_tx, ld, rx, clear, head):
    a = lax.axis_index("dp")
    g = lax.axis_index("ep")
    x = g // 2
    core = g % 2
    w, raw, dw = (wg, wu, wd), (raw_g, raw_u, raw_d), (dw_g, dw_u, dw_d)
    hs, ds, os_, wk = (hs_g, hs_u, hs_d), (ds_g, ds_u, ds_d), (os_g, os_u, os_d), (wk13, wk13, wk2)
    nexp, f = wg.shape[1], wg.shape[3]
    rows = tuple(r.shape[2] for r in raw)

    def expert(s, h):
        return jnp.clip(place[0, s] - h * nexp, 0, nexp - 1)

    def unit(t, k):
        return pl.ds(pl.multiple_of(k * rows[t], rows[t]), rows[t])

    def landing(t, j, k):
        if t == 2:
            return r2.at[j, unit(t, k)]
        return r13.at[j, unit(t, k), pl.ds(t * f, f)]

    def send(t, src, j, k, tx, ua, uep):
        return pltpu.make_async_remote_copy(
            src_ref=src, dst_ref=landing(t, j, k), send_sem=tx, recv_sem=rx.at[j, t],
            device_id={"dp": ua, "ep": uep}, device_id_type=pl.DeviceIdType.MESH)

    for c in range(2):

        @pl.when(core == c)
        def _(c=c):
            width = _pick(HUB[c], a)
            first = _pick(FIRST[c], a)
            slots = SLOTS[c]
            served = [_pick([SERVE[c][v][s[0]] for v in range(8)], a) for s in slots]

            def raw_copy(i, t):
                return pltpu.make_async_remote_copy(
                    src_ref=w[t].at[0, :, unit(t, first + i)], dst_ref=raw[t].at[i],
                    send_sem=raw_tx.at[t, i], recv_sem=raw_rx.at[t, i],
                    device_id={"dp": a, "ep": 2 * (1 - x) + c}, device_id_type=pl.DeviceIdType.MESH)

            def raw_start(i, _):
                for t in range(3):
                    raw_copy(i, t).start()
                return _

            if c == 1:
                pl.semaphore_wait(head, 1)
            lax.fori_loop(0, width, raw_start, 0)
            if c == 0:
                @pl.when(width > 0)
                def _():
                    raw_copy(0, 0).wait_send()

                pl.semaphore_signal(head, 1, device_id={"dp": a, "ep": 2 * x + 1}, device_id_type=pl.DeviceIdType.MESH)

            dslots = [[(s[1], s[2]) for s in slots if s[0] == u] if NDIR[c][u] else [] for u in range(8)]
            per = max(len(s) for s in dslots)
            count = _pick([max(len(s), 1) for s in dslots], a)
            ndir = _pick(NDIR[c], a)
            nranges = max(len(r) for r in DIRECT[c])
            starts, steps = [], []
            base = _pick([r[0][0] if r else 0 for r in DIRECT[c]], a)
            for q in range(1, nranges):
                starts.append(_pick([sum(hi - lo for lo, hi in r[:q]) if len(r) > q else 999 for r in DIRECT[c]], a))
                steps.append(_pick([r[q][0] - r[q - 1][1] if len(r) > q else 0 for r in DIRECT[c]], a))

            nown = _pick([UNITS if 2 in KIND[u][:2] else 0 for u in range(8)], a) if c == 1 else jnp.int32(0)
            njobs = nown + ndir

            def dunit(n):
                k = base + n
                for st, sp in zip(starts, steps):
                    k = k + jnp.where(n >= st, sp, 0)
                return k

            def junit(n):
                return jnp.where(n < nown, n, dunit(n - nown)) if c == 1 else dunit(n)

            def load(n, t):
                return pltpu.make_async_copy(w[t].at[0, :, unit(t, junit(n))], dw[t].at[n % 2], ld.at[t, n % 2])

            dtab = []
            for q in range(per):
                dtab.append((_pick([len(s) > q for s in dslots], a),
                             _pick([s[q][0] if len(s) > q else 0 for s in dslots], a),
                             _pick([s[q][1] if len(s) > q else 0 for s in dslots], a)))

            def dsend(n, t, q):
                _, uc, j = dtab[q]
                return send(t, ds[t].at[n * count + q], j, dunit(n), d_tx.at[t, n * count + q], a, 2 * (1 - x) + uc)

            def osend(n, t):
                return send(t, os_[t].at[n % ORING], 0, n, o_tx.at[t, n % ORING], a, 2 * x)

            @pl.when(njobs > 0)
            def _():
                for t in range(3):
                    load(0, t).start()

            def direct(n):
                for t in range(3):
                    load(n, t).wait()
                    wk[t][...] = dw[t][n % 2]

                    @pl.when(n + 1 < njobs)
                    def _():
                        load(n + 1, t).start()

                    @pl.when(n >= nown)
                    def _():
                        m = n - nown
                        for q in range(per):
                            on, uc, j = dtab[q]

                            @pl.when(on == 1)
                            def _():
                                e = expert((a * 4 + 2 * (1 - x) + uc) * 2 + j, 2 * x + c)
                                ds[t][m * count + q] = wk[t][e]

                        for q in range(per):

                            @pl.when(dtab[q][0] == 1)
                            def _():
                                dsend(m, t, q).start()

                    if c == 1:

                        @pl.when(n < nown)
                        def _():
                            @pl.when(n >= ORING)
                            def _():
                                osend(n - ORING, t).wait_send()

                            e = expert((a * 4 + 2 * x) * 2, 2 * x + c)
                            os_[t][n % ORING] = wk[t][e]
                            osend(n, t).start()

            def hub_copy(i, t, q):
                ua, uc, j = slots[q]
                src, tx = hs[t].at[i % RING, q], h_tx.at[t, i % RING, q]
                there = send(t, src, j, first + i, tx, ua, 2 * x + uc)
                here = pltpu.make_async_copy(src, landing(t, j, first + i), tx) if uc == c else None
                return there, here

            def hub_do(i, t, q, start):
                ua, uc, _ = slots[q]
                there, here = hub_copy(i, t, q)
                if here is None:
                    there.start() if start else there.wait_send()
                    return

                @pl.when(a == ua)
                def _():
                    here.start() if start else here.wait()

                @pl.when(a != ua)
                def _():
                    there.start() if start else there.wait_send()

            def hub_free(i, t):
                for q in range(len(slots)):

                    @pl.when(i < served[q])
                    def _():
                        hub_do(i, t, q, False)

            def hub(i):
                for t in range(3):

                    @pl.when(i >= RING)
                    def _():
                        hub_free(i - RING, t)

                    raw_copy(i, t).wait_recv()
                    wk[t][...] = raw[t][i]
                    for q in range(len(slots)):
                        ua, uc, j = slots[q]

                        @pl.when(i < served[q])
                        def _():
                            e = expert((ua * 4 + 2 * x + uc) * 2 + j, 2 * (1 - x) + c)
                            hs[t][i % RING, q] = wk[t][e]

                    for q in range(len(slots)):

                        @pl.when(i < served[q])
                        def _():
                            hub_do(i, t, q, True)

            def loop(lo, hi, f):
                lax.fori_loop(lo, hi, lambda i, s: (f(i), s)[1], 0)

            def mixed(i):
                @pl.when(i < width)
                def _():
                    hub(i)

                if c == 1:

                    @pl.when(i * OWN < nown)
                    def _():
                        loop(0, OWN, lambda r: direct(i * OWN + r))

            loop(0, jnp.maximum(width, _pick([UNITS // OWN if 2 in KIND[u][:2] else 0 for u in range(8)], a)) if c == 1 else width, mixed)

            def raw_drain(i):
                for t in range(3):
                    if c == 0 and t == 0:

                        @pl.when(i > 0)
                        def _():
                            raw_copy(i, 0).wait_send()
                    else:
                        raw_copy(i, t).wait_send()

            most = jnp.maximum(width - 1, 0)
            loop(0, most, raw_drain)
            pl.semaphore_signal(clear, 1, device_id={"dp": a, "ep": 2 * x + 1 - c},
                                device_id_type=pl.DeviceIdType.MESH)
            pl.semaphore_wait(clear, 1)
            loop(nown, njobs, direct)
            loop(most, width, raw_drain)

            def hub_drain(i, s):
                for t in range(3):
                    hub_free(i, t)
                return s

            lax.fori_loop(jnp.maximum(width - RING, 0), width, hub_drain, 0)

            def direct_drain(n, s):
                for t in range(3):
                    for q in range(per):

                        @pl.when(dtab[q][0] == 1)
                        def _():
                            dsend(n, t, q).wait_send()
                return s

            lax.fori_loop(0, ndir, direct_drain, 0)
            if c == 1:

                def own_drain(n, s):
                    for t in range(3):
                        osend(n, t).wait_send()
                    return s

                lax.fori_loop(jnp.maximum(nown - ORING, 0), nown, own_drain, 0)

            for u in range(8):

                @pl.when(a == u)
                def _(u=u):
                    for j in range(2):
                        kind = KIND[u][2 * c + j]
                        if kind == 3:
                            continue
                        n = UNITS - (SERVE[c][u][u] if kind == c else 0)
                        for t in range(3):
                            if t == 2:
                                part = r2.at[j, pl.ds(0, n * rows[2])]
                            else:
                                part = r13.at[j, pl.ds(0, n * rows[t]), pl.ds(t * f, f)]
                            pltpu.make_async_copy(part, part, rx.at[j, t]).wait()


def _local(nblk, place, wg, wu, wd, r13, r2, o13, o2, buf, lsem, ssem):
    a = lax.axis_index("dp")
    g = lax.axis_index("ep")
    nexp, f = wg.shape[1], wg.shape[3]
    b13 = r13.shape[1] // nblk[0]
    b2 = r2.shape[1] // nblk[1]
    n = 0
    jobs = []
    for j in range(2):
        own = jnp.int32(0)
        for u in range(8):
            for c in range(2):
                if KIND[u][2 * c + j] == 3:
                    own = jnp.where((a == u) & (g % 2 == c), 1, own)
        e = jnp.clip(place[0, (a * 4 + g) * 2 + j] - g * nexp, 0, nexp - 1)
        for b in range(nblk[0] + nblk[1]):
            jobs.append((n, j, b, own, e))
            n += 1
    for n, j, b, own, e in jobs:
        wide = b < nblk[0]
        r = pl.ds(b * b13, b13) if wide else pl.ds((b - nblk[0]) * b2, b2)

        @pl.when(own == 1)
        def _():
            if wide:
                pltpu.make_async_copy(wg.at[0, e, r], buf.at[n, :, pl.ds(0, f)], lsem.at[n]).start()
                pltpu.make_async_copy(wu.at[0, e, r], buf.at[n, :, pl.ds(f, f)], lsem.at[n]).start()
            else:
                pltpu.make_async_copy(wd.at[0, e, r], buf.at[n], lsem.at[n]).start()

        @pl.when(own == 0)
        def _():
            pltpu.make_async_copy((r13 if wide else r2).at[j, r], buf.at[n], lsem.at[n]).start()

    stores = []
    for n, j, b, own, e in jobs:
        wide = b < nblk[0]
        r = pl.ds(b * b13, b13) if wide else pl.ds((b - nblk[0]) * b2, b2)
        pltpu.make_async_copy(buf.at[n], buf.at[n], lsem.at[n]).wait()
        st = pltpu.make_async_copy(buf.at[n], (o13 if wide else o2).at[0, j, r], ssem.at[n])
        st.start()
        stores.append(st)
    for st in stores:
        st.wait()


def solution(mesh):
    anyspec = pl.BlockSpec(memory_space=pl.ANY)
    smem = pl.BlockSpec(memory_space=pltpu.SMEM)

    def body(wg, wu, wd, place):
        _, nexp, d, f = wg.shape
        dt = wg.dtype
        ra, rb = d // UNITS, f // UNITS
        wmax = max(max(h) for h in HUB)
        dma = pltpu.SemaphoreType.DMA

        def three(*lead):
            return [pltpu.VMEM((*lead, ra, f), dt), pltpu.VMEM((*lead, ra, f), dt), pltpu.VMEM((*lead, rb, d), dt)]

        r13, r2 = pl.pallas_call(
            _remote,
            out_shape=(jax.ShapeDtypeStruct((2, d, 2 * f), dt), jax.ShapeDtypeStruct((2, f, d), dt)),
            in_specs=[smem, anyspec, anyspec, anyspec],
            out_specs=(anyspec, anyspec),
            scratch_shapes=[
                *three(wmax, nexp), *three(2, nexp),
                pltpu.VMEM((nexp, ra, f), dt), pltpu.VMEM((nexp, rb, d), dt),
                *three(RING, MAXS), *three(DSTAGE), *three(ORING),
                dma((3, wmax)), dma((3, wmax)), dma((3, RING, MAXS)), dma((3, DSTAGE)), dma((3, ORING)),
                dma((3, 2)), dma((2, 3)), pltpu.SemaphoreType.REGULAR, pltpu.SemaphoreType.REGULAR,
            ],
            compiler_params=pltpu.CompilerParams(has_side_effects=True, vmem_limit_bytes=62 * 1024 * 1024),
            name="spread",
        )(place, wg, wu, wd)
        nblk = (8, 4)
        nbuf = 2 * sum(nblk)
        return pl.pallas_call(
            functools.partial(_local, nblk),
            out_shape=(jax.ShapeDtypeStruct((1, 2, d, 2 * f), dt), jax.ShapeDtypeStruct((1, 2, f, d), dt)),
            in_specs=[smem, anyspec, anyspec, anyspec, anyspec, anyspec],
            out_specs=(anyspec, anyspec),
            scratch_shapes=[pltpu.VMEM((nbuf, d // nblk[0], 2 * f), dt), dma((nbuf,)), dma((nbuf,))],
            compiler_params=pltpu.CompilerParams(vmem_limit_bytes=48 * 1024 * 1024),
            name="settle",
        )(place, wg, wu, wd, r13, r2)

    spec_in = P(None, "ep", None, None)
    spec_out = P(None, ("dp", "ep"), None, None)
    return jax.shard_map(body, mesh=mesh, in_specs=(spec_in, spec_in, spec_in, P(None, None)),
                         out_specs=(spec_out, spec_out), check_vma=False)
```

```python
import functools

import jax
import jax.numpy as jnp
from jax import lax
from jax.experimental import pallas as pl
from jax.experimental.pallas import tpu as pltpu
from jax.sharding import PartitionSpec as P

SUB = 1
UNITS = 32 * SUB
RING = 6 * SUB
ORING = 4
OWN = 8 * SUB
DSTAGE = 28 * SUB

def _rows(*digits):
    return tuple(tuple(SUB * int(d) for d in row) for row in digits)


HUB = _rows("56444405", "00666662")
FWD = _rows("00444400", "00000000")
THERE = (
    _rows("00000000", "00000000", "00004444", "00004434",
          "44440000", "44440000", "00000000", "00000000"),
    _rows(*[8 * "0"] * 8),
)
SERVE = (
    _rows("55532000", "66660600", "44440000", "44440000",
          "00004444", "00004444", "00000000", "00154555"),
    _rows("00000000", "00000000", "66666650", "46666600",
          "20666660", "04666660", "00606660", "00022220"),
)
KIND = []
for _a in range(8):
    _row = []
    for _c in range(2):
        for _j in range(2):
            _g = _c + 2
            _h = (2 * _a - _g) % 4 if _j < ((_a + 1) * 2) // 8 else (_g + _j + 1) % 4
            _row.append(_h if _h < 2 else (3 if _h == _g else 2))
    KIND.append(_row)
SLOTS = tuple(tuple((a, s // 2, s % 2) for a in range(8) for s in range(4) if KIND[a][s] == c) for c in range(2))
MAXS = max(len(s) for s in SLOTS)
ACROSS = tuple(2 * (3 - v // 2) + v % 2 for v in range(8))
FIRST = tuple(tuple(sum(HUB[c][:v]) for v in range(8)) for c in range(2))


def _direct(c, u):
    if not any(s[0] == u for s in SLOTS[c]):
        return []
    out = []
    parts = [(FIRST[c][v] + THERE[c][v][u] + SERVE[c][v][u], FIRST[c][v] + HUB[c][v]) for v in range(8)]
    for lo, hi in parts + [(sum(HUB[c]), UNITS)]:
        if lo == hi:
            continue
        if out and out[-1][1] == lo:
            out[-1][1] = hi
        else:
            out.append([lo, hi])
    return out


DIRECT = tuple(tuple(_direct(c, u) for u in range(8)) for c in range(2))
NDIR = tuple(tuple(sum(hi - lo for lo, hi in r) for r in DIRECT[c]) for c in range(2))


def _pick(table, i):
    r = jnp.int32(table[0])
    for k in range(1, len(table)):
        if table[k] != table[0]:
            r = lax.select(i == k, jnp.int32(table[k]), r)
    return r


def _remote(place, wg, wu, wd, r13, r2, raw_g, raw_u, raw_d, dw_g, dw_u, dw_d, wk13, wk2, hs_g, hs_u, hs_d,
            ds_g, ds_u, ds_d, os_g, os_u, os_d, raw_rx, raw_tx, h_tx, d_tx, o_tx, ld, rx, clear, head, f_tx):
    a = lax.axis_index("dp")
    g = lax.axis_index("ep")
    x = lax.div(g, 2)
    core = lax.rem(g, 2)
    w, raw, dw = (wg, wu, wd), (raw_g, raw_u, raw_d), (dw_g, dw_u, dw_d)
    hs, ds, os_, wk = (hs_g, hs_u, hs_d), (ds_g, ds_u, ds_d), (os_g, os_u, os_d), (wk13, wk13, wk2)
    nexp, f = wg.shape[1], wg.shape[3]
    rows = tuple(r.shape[2] for r in raw)

    def expert(s, h):
        return jnp.clip(place[0, s] - h * nexp, 0, nexp - 1)

    def unit(t, k):
        return pl.ds(pl.multiple_of(k * rows[t], rows[t]), rows[t])

    def landing(t, j, k):
        if t == 2:
            return r2.at[j, unit(t, k)]
        return r13.at[j, unit(t, k), pl.ds(t * f, f)]

    def send(t, src, j, k, tx, ua, uep):
        return pltpu.make_async_remote_copy(
            src_ref=src, dst_ref=landing(t, j, k), send_sem=tx, recv_sem=rx.at[j, t],
            device_id={"dp": ua, "ep": uep}, device_id_type=pl.DeviceIdType.MESH)

    for c in range(2):

        @pl.when(core == c)
        def _(c=c):
            width = _pick(HUB[c], a)
            first = _pick(FIRST[c], a)
            slots = SLOTS[c]
            nfwd = _pick(FWD[c], a)
            across = _pick(ACROSS, a)
            nmore = _pick([FWD[c][ACROSS[v]] for v in range(8)], a)
            wacross = _pick([HUB[c][ACROSS[v]] for v in range(8)], a)
            shift = _pick([FIRST[c][ACROSS[v]] - HUB[c][v] for v in range(8)], a)
            low = [_pick([THERE[c][v][s[0]] for v in range(8)], a) for s in slots]
            high = [_pick([THERE[c][v][s[0]] + SERVE[c][v][s[0]] for v in range(8)], a) for s in slots]
            more = [_pick([HUB[c][v] + THERE[c][ACROSS[v]][s[0]] for v in range(8)], a) for s in slots]

            def hunit(i):
                return lax.select(i < width, first, shift) + i

            def forward(i, t):
                return pltpu.make_async_remote_copy(
                    src_ref=raw[t].at[i], dst_ref=raw[t].at[wacross + i], send_sem=f_tx.at[t, i],
                    recv_sem=raw_rx.at[t, wacross + i],
                    device_id={"dp": across, "ep": g}, device_id_type=pl.DeviceIdType.MESH)

            def raw_copy(i, t):
                return pltpu.make_async_remote_copy(
                    src_ref=w[t].at[0, :, unit(t, first + i)], dst_ref=raw[t].at[i],
                    send_sem=raw_tx.at[t, i], recv_sem=raw_rx.at[t, i],
                    device_id={"dp": a, "ep": 2 * (1 - x) + c}, device_id_type=pl.DeviceIdType.MESH)

            def raw_start(i, _):
                for t in range(3):
                    raw_copy(i, t).start()
                return _

            if c == 1:
                pl.semaphore_wait(head, 1)
            lax.fori_loop(0, width, raw_start, 0)
            if c == 0:
                @pl.when(width > 0)
                def _():
                    raw_copy(0, 0).wait_send()

                pl.semaphore_signal(head, 1, device_id={"dp": a, "ep": 2 * x + 1}, device_id_type=pl.DeviceIdType.MESH)

            dslots = [[(s[1], s[2]) for s in slots if s[0] == u] if NDIR[c][u] else [] for u in range(8)]
            per = max(len(s) for s in dslots)
            count = _pick([max(len(s), 1) for s in dslots], a)
            ndir = _pick(NDIR[c], a)
            nranges = max(len(r) for r in DIRECT[c])
            starts, steps = [], []
            base = _pick([r[0][0] if r else 0 for r in DIRECT[c]], a)
            for q in range(1, nranges):
                starts.append(_pick([sum(hi - lo for lo, hi in r[:q]) if len(r) > q else 999 for r in DIRECT[c]], a))
                steps.append(_pick([r[q][0] - r[q - 1][1] if len(r) > q else 0 for r in DIRECT[c]], a))

            nown = _pick([UNITS if 2 in KIND[u][:2] else 0 for u in range(8)], a) if c == 1 else jnp.int32(0)
            njobs = nown + ndir

            def dunit(n):
                k = base + n
                for st, sp in zip(starts, steps):
                    k = k + lax.select(n >= st, sp, jnp.int32(0))
                return k

            def junit(n):
                return lax.select(n < nown, n, dunit(n - nown)) if c == 1 else dunit(n)

            def load(n, t):
                return pltpu.make_async_copy(w[t].at[0, :, unit(t, junit(n))], dw[t].at[lax.rem(n, 2)], ld.at[t, lax.rem(n, 2)])

            dtab = []
            for q in range(per):
                dtab.append((_pick([len(s) > q for s in dslots], a),
                             _pick([s[q][0] if len(s) > q else 0 for s in dslots], a),
                             _pick([s[q][1] if len(s) > q else 0 for s in dslots], a)))
                dtab[q] += (expert((a * 4 + 2 * (1 - x) + dtab[q][1]) * 2 + dtab[q][2], 2 * x + c),)
            eown = expert((a * 4 + 2 * x) * 2, 2 * x + c)

            def dsend(n, t, q):
                _, uc, j, _ = dtab[q]
                return send(t, ds[t].at[n * count + q], j, dunit(n), d_tx.at[t, n * count + q], a, 2 * (1 - x) + uc)

            def osend(n, t):
                return send(t, os_[t].at[lax.rem(n, ORING)], 0, n, o_tx.at[t, lax.rem(n, ORING)], a, 2 * x)

            @pl.when(njobs > 0)
            def _():
                for t in range(3):
                    load(0, t).start()

            def direct(n):
                for t in range(3):
                    load(n, t).wait()
                    wk[t][...] = dw[t][lax.rem(n, 2)]

                    @pl.when(n + 1 < njobs)
                    def _():
                        load(n + 1, t).start()

                    @pl.when(n >= nown)
                    def _():
                        m = n - nown
                        for q in range(per):
                            @pl.when(dtab[q][0] == 1)
                            def _():
                                e = dtab[q][3]
                                ds[t][m * count + q] = wk[t][e]

                        for q in range(per):

                            @pl.when(dtab[q][0] == 1)
                            def _():
                                dsend(m, t, q).start()

                    if c == 1:

                        @pl.when(n < nown)
                        def _():
                            @pl.when(n >= ORING)
                            def _():
                                osend(n - ORING, t).wait_send()

                            os_[t][lax.rem(n, ORING)] = wk[t][eown]
                            osend(n, t).start()

            picks = [expert((ua * 4 + 2 * x + uc) * 2 + j, 2 * (1 - x) + c) for ua, uc, j in slots]

            def serving(i):
                mine = i < width
                zero = jnp.int32(0)
                return [(i >= lax.select(mine, low[q], zero)) & (i < lax.select(mine, high[q], more[q]))
                        for q in range(len(slots))]

            def hub_do(p, k, t, q, start):
                ua, uc, j = slots[q]
                src, tx = hs[t].at[p, q], h_tx.at[t, p, q]

                def far():
                    cp = send(t, src, j, k, tx, ua, 2 * x + uc)
                    cp.start() if start else cp.wait_send()

                if uc != c:
                    far()
                    return
                pl.when(a != ua)(far)

                @pl.when(a == ua)
                def _():
                    cp = pltpu.make_async_copy(src, landing(t, j, k), tx)
                    cp.start() if start else cp.wait()

            def hub_free(i, on, p, t):
                k = hunit(i)
                for q in range(len(slots)):
                    pl.when(on[q])(functools.partial(hub_do, p, k, t, q, False))

            def hub(i):
                p = lax.rem(i, RING)
                k = hunit(i)
                on = serving(i)
                for t in range(3):

                    @pl.when(i >= RING)
                    def _():
                        hub_free(i - RING, serving(i - RING), p, t)

                    pltpu.make_async_copy(raw[t].at[i], raw[t].at[i], raw_rx.at[t, i]).wait()

                    @pl.when(i < nfwd)
                    def _():
                        forward(i, t).start()

                    wk[t][...] = raw[t][i]
                    for q in range(len(slots)):

                        @pl.when(on[q])
                        def _():
                            hs[t][p, q] = wk[t][picks[q]]

                    for q in range(len(slots)):
                        pl.when(on[q])(functools.partial(hub_do, p, k, t, q, True))

            def loop(lo, hi, f):
                lax.fori_loop(lo, hi, lambda i, s: (f(i), s)[1], 0)

            def raw_drain(i):
                for t in range(3):
                    if c == 0 and t == 0:

                        @pl.when(i > 0)
                        def _():
                            raw_copy(i, 0).wait_send()
                    else:
                        raw_copy(i, t).wait_send()

            most = jnp.maximum(width - 1, 0)
            early = _pick((0, 0, 1, 1, 1, 1, 0, 0), a)

            def drain_most(i):
                @pl.when(i < most)
                def _():
                    raw_drain(i)

            def direct_some(n):
                @pl.when(n < njobs)
                def _():
                    direct(n)

            def mixed(i):
                @pl.when(i == most)
                def _():
                    loop(0, max(HUB[c]) - 1, drain_most)
                    pl.semaphore_signal(clear, 1, device_id={"dp": a, "ep": 2 * x + 1 - c},
                                        device_id_type=pl.DeviceIdType.MESH)
                    if c == 0:

                        @pl.when(early == 1)
                        def _():
                            loop(0, max(NDIR[0]), direct_some)

                def pair(r):
                    @pl.when(i < lax.select(r == 0, width, nmore))
                    def _():
                        hub(i + r * width)

                loop(0, 2, pair)
                if c == 1:

                    @pl.when(i * OWN < nown)
                    def _():
                        loop(0, OWN, lambda r: direct(i * OWN + r))

            ntimes = [max(HUB[c][v], FWD[c][ACROSS[v]], UNITS // OWN if c == 1 and 2 in KIND[v][:2] else 1) for v in range(8)]
            loop(0, _pick(ntimes, a), mixed)

            if c == 0:

                @pl.when(early == 0)
                def _():
                    pl.semaphore_wait(clear, 1)
                    loop(nown, njobs, direct)

                @pl.when(early == 1)
                def _():
                    pl.semaphore_wait(clear, 1)
            else:
                pl.semaphore_wait(clear, 1)
                loop(nown, njobs, direct)
            loop(most, width, raw_drain)

            def forward_drain(i):
                for t in range(3):
                    forward(i, t).wait_send()

            loop(0, nfwd, forward_drain)

            def hub_drain(i, s):
                on = serving(i)
                for t in range(3):
                    hub_free(i, on, lax.rem(i, RING), t)
                return s

            lax.fori_loop(jnp.maximum(width + nmore - RING, 0), width + nmore, hub_drain, 0)

            def direct_drain(n, s):
                for t in range(3):
                    for q in range(per):

                        @pl.when(dtab[q][0] == 1)
                        def _():
                            dsend(n, t, q).wait_send()
                return s

            lax.fori_loop(0, ndir, direct_drain, 0)
            if c == 1:

                def own_drain(n, s):
                    for t in range(3):
                        osend(n, t).wait_send()
                    return s

                lax.fori_loop(jnp.maximum(nown - ORING, 0), nown, own_drain, 0)

            for u in range(8):

                @pl.when(a == u)
                def _(u=u):
                    for j in range(2):
                        kind = KIND[u][2 * c + j]
                        if kind == 3:
                            continue
                        n = UNITS - (SERVE[c][u][u] + THERE[c][ACROSS[u]][u] if kind == c else 0)
                        for t in range(3):
                            if t == 2:
                                part = r2.at[j, pl.ds(0, n * rows[2])]
                            else:
                                part = r13.at[j, pl.ds(0, n * rows[t]), pl.ds(t * f, f)]
                            pltpu.make_async_copy(part, part, rx.at[j, t]).wait()


def _local(nblk, place, wg, wu, wd, r13, r2, o13, o2, buf, lsem, ssem):
    a = lax.axis_index("dp")
    g = lax.axis_index("ep")
    nexp, f = wg.shape[1], wg.shape[3]
    b13 = r13.shape[1] // nblk[0]
    b2 = r2.shape[1] // nblk[1]
    n = 0
    jobs = []
    for j in range(2):
        own = jnp.int32(0)
        for u in range(8):
            for c in range(2):
                if KIND[u][2 * c + j] == 3:
                    own = jnp.where((a == u) & (g % 2 == c), 1, own)
        e = jnp.clip(place[0, (a * 4 + g) * 2 + j] - g * nexp, 0, nexp - 1)
        for b in range(nblk[0] + nblk[1]):
            jobs.append((n, j, b, own, e))
            n += 1
    for n, j, b, own, e in jobs:
        wide = b < nblk[0]
        r = pl.ds(b * b13, b13) if wide else pl.ds((b - nblk[0]) * b2, b2)

        @pl.when(own == 1)
        def _():
            if wide:
                pltpu.make_async_copy(wg.at[0, e, r], buf.at[n, :, pl.ds(0, f)], lsem.at[n]).start()
                pltpu.make_async_copy(wu.at[0, e, r], buf.at[n, :, pl.ds(f, f)], lsem.at[n]).start()
            else:
                pltpu.make_async_copy(wd.at[0, e, r], buf.at[n], lsem.at[n]).start()

        @pl.when(own == 0)
        def _():
            pltpu.make_async_copy((r13 if wide else r2).at[j, r], buf.at[n], lsem.at[n]).start()

    stores = []
    for n, j, b, own, e in jobs:
        wide = b < nblk[0]
        r = pl.ds(b * b13, b13) if wide else pl.ds((b - nblk[0]) * b2, b2)
        pltpu.make_async_copy(buf.at[n], buf.at[n], lsem.at[n]).wait()
        st = pltpu.make_async_copy(buf.at[n], (o13 if wide else o2).at[0, j, r], ssem.at[n])
        st.start()
        stores.append(st)
    for st in stores:
        st.wait()


def solution(mesh):
    anyspec = pl.BlockSpec(memory_space=pl.ANY)
    smem = pl.BlockSpec(memory_space=pltpu.SMEM)

    def body(wg, wu, wd, place):
        _, nexp, d, f = wg.shape
        dt = wg.dtype
        ra, rb = d // UNITS, f // UNITS
        wmax = max(HUB[c][v] + FWD[c][ACROSS[v]] for c in range(2) for v in range(8))
        dma = pltpu.SemaphoreType.DMA

        def three(*lead):
            return [pltpu.VMEM((*lead, ra, f), dt), pltpu.VMEM((*lead, ra, f), dt), pltpu.VMEM((*lead, rb, d), dt)]

        r13, r2 = pl.pallas_call(
            _remote,
            out_shape=(jax.ShapeDtypeStruct((2, d, 2 * f), dt), jax.ShapeDtypeStruct((2, f, d), dt)),
            in_specs=[smem, anyspec, anyspec, anyspec],
            out_specs=(anyspec, anyspec),
            scratch_shapes=[
                *three(wmax, nexp), *three(2, nexp),
                pltpu.VMEM((nexp, ra, f), dt), pltpu.VMEM((nexp, rb, d), dt),
                *three(RING, MAXS), *three(DSTAGE), *three(ORING),
                dma((3, wmax)), dma((3, wmax)), dma((3, RING, MAXS)), dma((3, DSTAGE)), dma((3, ORING)),
                dma((3, 2)), dma((2, 3)), pltpu.SemaphoreType.REGULAR, pltpu.SemaphoreType.REGULAR, dma((3, wmax)),
            ],
            compiler_params=pltpu.CompilerParams(has_side_effects=True, vmem_limit_bytes=62 * 1024 * 1024),
            name="spread",
        )(place, wg, wu, wd)
        nblk = (8, 4)
        nbuf = 2 * sum(nblk)
        return pl.pallas_call(
            functools.partial(_local, nblk),
            out_shape=(jax.ShapeDtypeStruct((1, 2, d, 2 * f), dt), jax.ShapeDtypeStruct((1, 2, f, d), dt)),
            in_specs=[smem, anyspec, anyspec, anyspec, anyspec, anyspec],
            out_specs=(anyspec, anyspec),
            scratch_shapes=[pltpu.VMEM((nbuf, d // nblk[0], 2 * f), dt), dma((nbuf,)), dma((nbuf,))],
            compiler_params=pltpu.CompilerParams(vmem_limit_bytes=48 * 1024 * 1024),
            name="settle",
        )(place, wg, wu, wd, r13, r2)

    spec_in = P(None, "ep", None, None)
    spec_out = P(None, ("dp", "ep"), None, None)
    return jax.shard_map(body, mesh=mesh, in_specs=(spec_in, spec_in, spec_in, P(None, None)),
                         out_specs=(spec_out, spec_out), check_vma=False)
```

```python
import functools

import jax
import jax.numpy as jnp
from jax import lax
from jax.experimental import pallas as pl
from jax.experimental.pallas import tpu as pltpu
from jax.sharding import PartitionSpec as P

SUB = 1
UNITS = 32 * SUB
RING = 4 * SUB
ORING = 4
OWN = 8 * SUB
DSTAGE = 28 * SUB

def _rows(*digits):
    return tuple(tuple(SUB * int(d) for d in row) for row in digits)


HUB = _rows("56444405", "00666662")
FWD = _rows("00444400", "00000000")
THERE = (
    _rows("00000000", "00000000", "00004444", "00004434",
          "44440000", "44440000", "00000000", "00000000"),
    _rows(*[8 * "0"] * 8),
)
SERVE = (
    _rows("55532000", "66660600", "44440000", "44440000",
          "00004444", "00004444", "00000000", "00154555"),
    _rows("00000000", "00000000", "66666650", "46666600",
          "20666660", "04666660", "00606660", "00022220"),
)
KIND = []
for _a in range(8):
    _row = []
    for _c in range(2):
        for _j in range(2):
            _g = _c + 2
            _h = (2 * _a - _g) % 4 if _j < ((_a + 1) * 2) // 8 else (_g + _j + 1) % 4
            _row.append(_h if _h < 2 else (3 if _h == _g else 2))
    KIND.append(_row)
SLOTS = tuple(tuple((a, s // 2, s % 2) for a in range(8) for s in range(4) if KIND[a][s] == c) for c in range(2))
MAXS = max(len(s) for s in SLOTS)
ACROSS = tuple(2 * (3 - v // 2) + v % 2 for v in range(8))
FIRST = tuple(tuple(sum(HUB[c][:v]) for v in range(8)) for c in range(2))


def _direct(c, u):
    if not any(s[0] == u for s in SLOTS[c]):
        return []
    out = []
    parts = [(FIRST[c][v] + THERE[c][v][u] + SERVE[c][v][u], FIRST[c][v] + HUB[c][v]) for v in range(8)]
    for lo, hi in parts + [(sum(HUB[c]), UNITS)]:
        if lo == hi:
            continue
        if out and out[-1][1] == lo:
            out[-1][1] = hi
        else:
            out.append([lo, hi])
    return out


DIRECT = tuple(tuple(_direct(c, u) for u in range(8)) for c in range(2))
NDIR = tuple(tuple(sum(hi - lo for lo, hi in r) for r in DIRECT[c]) for c in range(2))


def _pick(table, i):
    r = jnp.int32(table[0])
    for k in range(1, len(table)):
        if table[k] != table[0]:
            r = lax.select(i == k, jnp.int32(table[k]), r)
    return r


def _remote(place, wg, wu, wd, r13, r2, raw_g, raw_u, raw_d, dw_g, dw_u, dw_d, wk13, wk2, hs_g, hs_u, hs_d,
            ds_g, ds_u, ds_d, os_g, os_u, os_d, raw_rx, raw_tx, h_tx, d_tx, o_tx, ld, rx, clear, head, f_tx, ready):
    a = lax.axis_index("dp")
    g = lax.axis_index("ep")
    x = lax.div(g, 2)
    core = lax.rem(g, 2)
    w, raw, dw = (wg, wu, wd), (raw_g, raw_u, raw_d), (dw_g, dw_u, dw_d)
    hs, ds, os_, wk = (hs_g, hs_u, hs_d), (ds_g, ds_u, ds_d), (os_g, os_u, os_d), (wk13, wk13, wk2)
    nexp, f = wg.shape[1], wg.shape[3]
    rows = tuple(r.shape[2] for r in raw)

    def expert(s, h):
        return jnp.clip(place[0, s] - h * nexp, 0, nexp - 1)

    def unit(t, k):
        return pl.ds(pl.multiple_of(k * rows[t], rows[t]), rows[t])

    def landing(t, j, k):
        if t == 2:
            return r2.at[j, unit(t, k)]
        return r13.at[j, unit(t, k), pl.ds(t * f, f)]

    def send(t, src, j, k, tx, ua, uep):
        return pltpu.make_async_remote_copy(
            src_ref=src, dst_ref=landing(t, j, k), send_sem=tx, recv_sem=rx.at[j, t],
            device_id={"dp": ua, "ep": uep}, device_id_type=pl.DeviceIdType.MESH)

    z, y = lax.div(a, 2), lax.rem(a, 2)

    def tell(sem, dp, ep):
        pl.semaphore_signal(sem, 1, device_id={"dp": dp, "ep": ep}, device_id_type=pl.DeviceIdType.MESH)

    def tell_z(sem):
        @pl.when(z > 0)
        def _():
            tell(sem, a - 2, g)

        @pl.when(z < 3)
        def _():
            tell(sem, a + 2, g)

    nz = _pick((1, 2, 2, 1), z)

    barrier = pltpu.get_barrier_semaphore()
    other = 2 * x + 1 - core
    tell(barrier, a, 2 - 2 * x)
    tell(barrier, a, 3 - 2 * x)
    tell(barrier, a, other)
    tell(barrier, 2 * z + 1 - y, g)
    tell_z(barrier)
    pl.semaphore_wait(barrier, 4 + nz)

    def meet():
        for r in range(2):
            tell_z(ready.at[r])
            pl.semaphore_wait(ready.at[r], nz)
        tell(ready.at[2], 2 * z + 1 - y, g)
        pl.semaphore_wait(ready.at[2], 1)
        tell(ready.at[3], a, other)
        pl.semaphore_wait(ready.at[3], 1)

    for c in range(2):

        @pl.when(core == c)
        def _(c=c):
            width = _pick(HUB[c], a)
            first = _pick(FIRST[c], a)
            slots = SLOTS[c]
            nfwd = _pick(FWD[c], a)
            across = _pick(ACROSS, a)
            nmore = _pick([FWD[c][ACROSS[v]] for v in range(8)], a)
            wacross = _pick([HUB[c][ACROSS[v]] for v in range(8)], a)
            shift = _pick([FIRST[c][ACROSS[v]] - HUB[c][v] for v in range(8)], a)
            low = [_pick([THERE[c][v][s[0]] for v in range(8)], a) for s in slots]
            high = [_pick([THERE[c][v][s[0]] + SERVE[c][v][s[0]] for v in range(8)], a) for s in slots]
            more = [_pick([HUB[c][v] + THERE[c][ACROSS[v]][s[0]] for v in range(8)], a) for s in slots]

            def hunit(i):
                return lax.select(i < width, first, shift) + i

            def forward(i, t):
                return pltpu.make_async_remote_copy(
                    src_ref=raw[t].at[i], dst_ref=raw[t].at[wacross + i], send_sem=f_tx.at[t, i],
                    recv_sem=raw_rx.at[t, wacross + i],
                    device_id={"dp": across, "ep": g}, device_id_type=pl.DeviceIdType.MESH)

            def raw_copy(i, t):
                return pltpu.make_async_remote_copy(
                    src_ref=w[t].at[0, :, unit(t, first + i)], dst_ref=raw[t].at[i],
                    send_sem=raw_tx.at[t, i], recv_sem=raw_rx.at[t, i],
                    device_id={"dp": a, "ep": 2 * (1 - x) + c}, device_id_type=pl.DeviceIdType.MESH)

            def raw_start(i, _):
                for t in range(3):
                    raw_copy(i, t).start()
                return _

            if c == 0:
                lax.fori_loop(0, width, raw_start, 0)
                meet()

                @pl.when(width > 0)
                def _():
                    raw_copy(0, 0).wait_send()

                tell(head, a, g + 1)
            else:
                meet()
                pl.semaphore_wait(head, 1)
                lax.fori_loop(0, width, raw_start, 0)

            dslots = [[(s[1], s[2]) for s in slots if s[0] == u] if NDIR[c][u] else [] for u in range(8)]
            per = max(len(s) for s in dslots)
            count = _pick([max(len(s), 1) for s in dslots], a)
            ndir = _pick(NDIR[c], a)
            nranges = max(len(r) for r in DIRECT[c])
            starts, steps = [], []
            base = _pick([r[0][0] if r else 0 for r in DIRECT[c]], a)
            for q in range(1, nranges):
                starts.append(_pick([sum(hi - lo for lo, hi in r[:q]) if len(r) > q else 999 for r in DIRECT[c]], a))
                steps.append(_pick([r[q][0] - r[q - 1][1] if len(r) > q else 0 for r in DIRECT[c]], a))

            nown = _pick([UNITS if 2 in KIND[u][:2] else 0 for u in range(8)], a) if c == 1 else jnp.int32(0)
            njobs = nown + ndir

            def dunit(n):
                k = base + n
                for st, sp in zip(starts, steps):
                    k = k + lax.select(n >= st, sp, jnp.int32(0))
                return k

            def junit(n):
                return lax.select(n < nown, n, dunit(n - nown)) if c == 1 else dunit(n)

            def load(n, t):
                return pltpu.make_async_copy(w[t].at[0, :, unit(t, junit(n))], dw[t].at[lax.rem(n, 2)], ld.at[t, lax.rem(n, 2)])

            dtab = []
            for q in range(per):
                dtab.append((_pick([len(s) > q for s in dslots], a),
                             _pick([s[q][0] if len(s) > q else 0 for s in dslots], a),
                             _pick([s[q][1] if len(s) > q else 0 for s in dslots], a)))
                dtab[q] += (expert((a * 4 + 2 * (1 - x) + dtab[q][1]) * 2 + dtab[q][2], 2 * x + c),)
            eown = expert((a * 4 + 2 * x) * 2, 2 * x + c)

            def dsend(n, t, q):
                _, uc, j, _ = dtab[q]
                return send(t, ds[t].at[n * count + q], j, dunit(n), d_tx.at[t, n * count + q], a, 2 * (1 - x) + uc)

            def osend(n, t):
                return send(t, os_[t].at[lax.rem(n, ORING)], 0, n, o_tx.at[t, lax.rem(n, ORING)], a, 2 * x)

            @pl.when(njobs > 0)
            def _():
                for t in range(3):
                    load(0, t).start()

            def direct(n):
                for t in range(3):
                    load(n, t).wait()
                    wk[t][...] = dw[t][lax.rem(n, 2)]

                    @pl.when(n + 1 < njobs)
                    def _():
                        load(n + 1, t).start()

                    @pl.when(n >= nown)
                    def _():
                        m = n - nown
                        for q in range(per):
                            @pl.when(dtab[q][0] == 1)
                            def _():
                                e = dtab[q][3]
                                ds[t][m * count + q] = wk[t][e]

                        for q in range(per):

                            @pl.when(dtab[q][0] == 1)
                            def _():
                                dsend(m, t, q).start()

                    if c == 1:

                        @pl.when(n < nown)
                        def _():
                            @pl.when(n >= ORING)
                            def _():
                                osend(n - ORING, t).wait_send()

                            os_[t][lax.rem(n, ORING)] = wk[t][eown]
                            osend(n, t).start()

            picks = [expert((ua * 4 + 2 * x + uc) * 2 + j, 2 * (1 - x) + c) for ua, uc, j in slots]

            def serving(i):
                mine = i < width
                zero = jnp.int32(0)
                return [(i >= lax.select(mine, low[q], zero)) & (i < lax.select(mine, high[q], more[q]))
                        for q in range(len(slots))]

            def hub_do(p, k, t, q, start):
                ua, uc, j = slots[q]
                src, tx = hs[t].at[p, q], h_tx.at[t, p, q]

                def far():
                    cp = send(t, src, j, k, tx, ua, 2 * x + uc)
                    cp.start() if start else cp.wait_send()

                if uc != c:
                    far()
                    return
                pl.when(a != ua)(far)

                @pl.when(a == ua)
                def _():
                    cp = pltpu.make_async_copy(src, landing(t, j, k), tx)
                    cp.start() if start else cp.wait()

            def hub_free(i, on, p, t):
                k = hunit(i)
                for q in range(len(slots)):
                    pl.when(on[q])(functools.partial(hub_do, p, k, t, q, False))

            def hub(i):
                p = lax.rem(i, RING)
                k = hunit(i)
                on = serving(i)
                for t in range(3):

                    @pl.when(i >= RING)
                    def _():
                        hub_free(i - RING, serving(i - RING), p, t)

                    pltpu.make_async_copy(raw[t].at[i], raw[t].at[i], raw_rx.at[t, i]).wait()

                    @pl.when(i < nfwd)
                    def _():
                        forward(i, t).start()

                    wk[t][...] = raw[t][i]
                    for q in range(len(slots)):

                        @pl.when(on[q])
                        def _():
                            hs[t][p, q] = wk[t][picks[q]]

                    for q in range(len(slots)):
                        pl.when(on[q])(functools.partial(hub_do, p, k, t, q, True))

            def loop(lo, hi, f):
                lax.fori_loop(lo, hi, lambda i, s: (f(i), s)[1], 0)

            def raw_drain(i):
                for t in range(3):
                    if c == 0 and t == 0:

                        @pl.when(i > 0)
                        def _():
                            raw_copy(i, 0).wait_send()
                    else:
                        raw_copy(i, t).wait_send()

            most = jnp.maximum(width - 1, 0)
            early = _pick((0, 0, 1, 1, 1, 1, 0, 0), a)

            def drain_most(i):
                @pl.when(i < most)
                def _():
                    raw_drain(i)

            def direct_some(n):
                @pl.when(n < njobs)
                def _():
                    direct(n)

            def mixed(i):
                @pl.when(i == most)
                def _():
                    loop(0, max(HUB[c]) - 1, drain_most)
                    pl.semaphore_signal(clear, 1, device_id={"dp": a, "ep": 2 * x + 1 - c},
                                        device_id_type=pl.DeviceIdType.MESH)
                    if c == 0:

                        @pl.when(early == 1)
                        def _():
                            loop(0, max(NDIR[0]), direct_some)

                def pair(r):
                    @pl.when(i < lax.select(r == 0, width, nmore))
                    def _():
                        hub(i + r * width)

                loop(0, 2, pair)
                if c == 1:

                    @pl.when(i * OWN < nown)
                    def _():
                        loop(0, OWN, lambda r: direct(i * OWN + r))

            ntimes = [max(HUB[c][v], FWD[c][ACROSS[v]], UNITS // OWN if c == 1 and 2 in KIND[v][:2] else 1) for v in range(8)]
            loop(0, _pick(ntimes, a), mixed)

            if c == 0:

                @pl.when(early == 0)
                def _():
                    pl.semaphore_wait(clear, 1)
                    loop(nown, njobs, direct)

                @pl.when(early == 1)
                def _():
                    pl.semaphore_wait(clear, 1)
            else:
                pl.semaphore_wait(clear, 1)
                loop(nown, njobs, direct)
            loop(most, width, raw_drain)

            def forward_drain(i):
                for t in range(3):
                    forward(i, t).wait_send()

            loop(0, nfwd, forward_drain)

            def hub_drain(i, s):
                on = serving(i)
                for t in range(3):
                    hub_free(i, on, lax.rem(i, RING), t)
                return s

            lax.fori_loop(jnp.maximum(width + nmore - RING, 0), width + nmore, hub_drain, 0)

            def direct_drain(n, s):
                for t in range(3):
                    for q in range(per):

                        @pl.when(dtab[q][0] == 1)
                        def _():
                            dsend(n, t, q).wait_send()
                return s

            lax.fori_loop(0, ndir, direct_drain, 0)
            if c == 1:

                def own_drain(n, s):
                    for t in range(3):
                        osend(n, t).wait_send()
                    return s

                lax.fori_loop(jnp.maximum(nown - ORING, 0), nown, own_drain, 0)

            for u in range(8):

                @pl.when(a == u)
                def _(u=u):
                    for j in range(2):
                        kind = KIND[u][2 * c + j]
                        if kind == 3:
                            continue
                        n = UNITS - (SERVE[c][u][u] + THERE[c][ACROSS[u]][u] if kind == c else 0)
                        for t in range(3):
                            if t == 2:
                                part = r2.at[j, pl.ds(0, n * rows[2])]
                            else:
                                part = r13.at[j, pl.ds(0, n * rows[t]), pl.ds(t * f, f)]
                            pltpu.make_async_copy(part, part, rx.at[j, t]).wait()


def _local(nblk, place, wg, wu, wd, r13, r2, o13, o2, buf, lsem, ssem):
    a = lax.axis_index("dp")
    g = lax.axis_index("ep")
    nexp, f = wg.shape[1], wg.shape[3]
    b13 = r13.shape[1] // nblk[0]
    b2 = r2.shape[1] // nblk[1]
    n = 0
    jobs = []
    for j in range(2):
        own = jnp.int32(0)
        for u in range(8):
            for c in range(2):
                if KIND[u][2 * c + j] == 3:
                    own = jnp.where((a == u) & (g % 2 == c), 1, own)
        e = jnp.clip(place[0, (a * 4 + g) * 2 + j] - g * nexp, 0, nexp - 1)
        for b in range(nblk[0] + nblk[1]):
            jobs.append((n, j, b, own, e))
            n += 1
    for n, j, b, own, e in jobs:
        wide = b < nblk[0]
        r = pl.ds(b * b13, b13) if wide else pl.ds((b - nblk[0]) * b2, b2)

        @pl.when(own == 1)
        def _():
            if wide:
                pltpu.make_async_copy(wg.at[0, e, r], buf.at[n, :, pl.ds(0, f)], lsem.at[n]).start()
                pltpu.make_async_copy(wu.at[0, e, r], buf.at[n, :, pl.ds(f, f)], lsem.at[n]).start()
            else:
                pltpu.make_async_copy(wd.at[0, e, r], buf.at[n], lsem.at[n]).start()

        @pl.when(own == 0)
        def _():
            pltpu.make_async_copy((r13 if wide else r2).at[j, r], buf.at[n], lsem.at[n]).start()

    stores = []
    for n, j, b, own, e in jobs:
        wide = b < nblk[0]
        r = pl.ds(b * b13, b13) if wide else pl.ds((b - nblk[0]) * b2, b2)
        pltpu.make_async_copy(buf.at[n], buf.at[n], lsem.at[n]).wait()
        st = pltpu.make_async_copy(buf.at[n], (o13 if wide else o2).at[0, j, r], ssem.at[n])
        st.start()
        stores.append(st)
    for st in stores:
        st.wait()


def solution(mesh):
    anyspec = pl.BlockSpec(memory_space=pl.ANY)
    smem = pl.BlockSpec(memory_space=pltpu.SMEM)

    def body(wg, wu, wd, place):
        _, nexp, d, f = wg.shape
        dt = wg.dtype
        ra, rb = d // UNITS, f // UNITS
        wmax = max(HUB[c][v] + FWD[c][ACROSS[v]] for c in range(2) for v in range(8))
        dma = pltpu.SemaphoreType.DMA

        def three(*lead):
            return [pltpu.VMEM((*lead, ra, f), dt), pltpu.VMEM((*lead, ra, f), dt), pltpu.VMEM((*lead, rb, d), dt)]

        r13, r2 = pl.pallas_call(
            _remote,
            out_shape=(jax.ShapeDtypeStruct((2, d, 2 * f), dt), jax.ShapeDtypeStruct((2, f, d), dt)),
            in_specs=[smem, anyspec, anyspec, anyspec],
            out_specs=(anyspec, anyspec),
            scratch_shapes=[
                *three(wmax, nexp), *three(2, nexp),
                pltpu.VMEM((nexp, ra, f), dt), pltpu.VMEM((nexp, rb, d), dt),
                *three(RING, MAXS), *three(DSTAGE), *three(ORING),
                dma((3, wmax)), dma((3, wmax)), dma((3, RING, MAXS)), dma((3, DSTAGE)), dma((3, ORING)),
                dma((3, 2)), dma((2, 3)), pltpu.SemaphoreType.REGULAR, pltpu.SemaphoreType.REGULAR, dma((3, wmax)),
                pltpu.SemaphoreType.REGULAR((4,)),
            ],
            compiler_params=pltpu.CompilerParams(has_side_effects=True, collective_id=0, vmem_limit_bytes=62 * 1024 * 1024),
            name="spread",
        )(place, wg, wu, wd)
        nblk = (8, 4)
        nbuf = 2 * sum(nblk)
        return pl.pallas_call(
            functools.partial(_local, nblk),
            out_shape=(jax.ShapeDtypeStruct((1, 2, d, 2 * f), dt), jax.ShapeDtypeStruct((1, 2, f, d), dt)),
            in_specs=[smem, anyspec, anyspec, anyspec, anyspec, anyspec],
            out_specs=(anyspec, anyspec),
            scratch_shapes=[pltpu.VMEM((nbuf, d // nblk[0], 2 * f), dt), dma((nbuf,)), dma((nbuf,))],
            compiler_params=pltpu.CompilerParams(vmem_limit_bytes=48 * 1024 * 1024),
            name="settle",
        )(place, wg, wu, wd, r13, r2)

    spec_in = P(None, "ep", None, None)
    spec_out = P(None, ("dp", "ep"), None, None)
    return jax.shard_map(body, mesh=mesh, in_specs=(spec_in, spec_in, spec_in, P(None, None)),
                         out_specs=(spec_out, spec_out), check_vma=False)
```

```python
import functools

import jax
import jax.numpy as jnp
from jax import lax
from jax.experimental import pallas as pl
from jax.experimental.pallas import tpu as pltpu
from jax.sharding import PartitionSpec as P

SUB = 1
UNITS = 32 * SUB
RING = 4 * SUB
ORING = 4
OWN = 8 * SUB
DSTAGE = 28 * SUB

def _rows(*digits):
    return tuple(tuple(SUB * int(d) for d in row) for row in digits)


HUB = _rows("56444405", "00666662")
FWD = _rows("00444400", "00000000")
THERE = (
    _rows("00000000", "00000000", "00004444", "00004434",
          "44440000", "44440000", "00000000", "00000000"),
    _rows(*[8 * "0"] * 8),
)
SERVE = (
    _rows("55532000", "66660600", "44440000", "44440000",
          "00004444", "00004444", "00000000", "00154555"),
    _rows("00000000", "00000000", "66666650", "46666600",
          "20666660", "04666660", "00606660", "00022220"),
)
KIND = []
for _a in range(8):
    _row = []
    for _c in range(2):
        for _j in range(2):
            _g = _c + 2
            _h = (2 * _a - _g) % 4 if _j < ((_a + 1) * 2) // 8 else (_g + _j + 1) % 4
            _row.append(_h if _h < 2 else (3 if _h == _g else 2))
    KIND.append(_row)
SLOTS = tuple(tuple((a, s // 2, s % 2) for a in range(8) for s in range(4) if KIND[a][s] == c) for c in range(2))
MAXS = max(len(s) for s in SLOTS)
ACROSS = tuple(2 * (3 - v // 2) + v % 2 for v in range(8))
FIRST = tuple(tuple(sum(HUB[c][:v]) for v in range(8)) for c in range(2))


def _direct(c, u):
    if not any(s[0] == u for s in SLOTS[c]):
        return []
    out = []
    parts = [(FIRST[c][v] + THERE[c][v][u] + SERVE[c][v][u], FIRST[c][v] + HUB[c][v]) for v in range(8)]
    for lo, hi in parts + [(sum(HUB[c]), UNITS)]:
        if lo == hi:
            continue
        if out and out[-1][1] == lo:
            out[-1][1] = hi
        else:
            out.append([lo, hi])
    return out


DIRECT = tuple(tuple(_direct(c, u) for u in range(8)) for c in range(2))
NDIR = tuple(tuple(sum(hi - lo for lo, hi in r) for r in DIRECT[c]) for c in range(2))


def _pick(table, i):
    r = jnp.int32(table[0])
    for k in range(1, len(table)):
        if table[k] != table[0]:
            r = lax.select(i == k, jnp.int32(table[k]), r)
    return r


def _remote(place, wg, wu, wd, r13, r2, raw_g, raw_u, raw_d, dw_g, dw_u, dw_d, wk13, wk2, hs_g, hs_u, hs_d,
            ds_g, ds_u, ds_d, os_g, os_u, os_d, raw_rx, raw_tx, h_tx, d_tx, o_tx, ld, rx, clear, head, f_tx, ready):
    a = lax.axis_index("dp")
    g = lax.axis_index("ep")
    x = lax.div(g, 2)
    core = lax.rem(g, 2)
    w, raw, dw = (wg, wu, wd), (raw_g, raw_u, raw_d), (dw_g, dw_u, dw_d)
    hs, ds, os_, wk = (hs_g, hs_u, hs_d), (ds_g, ds_u, ds_d), (os_g, os_u, os_d), (wk13, wk13, wk2)
    nexp, f = wg.shape[1], wg.shape[3]
    rows = tuple(r.shape[2] for r in raw)

    def expert(s, h):
        return jnp.clip(place[0, s] - h * nexp, 0, nexp - 1)

    def unit(t, k):
        return pl.ds(pl.multiple_of(k * rows[t], rows[t]), rows[t])

    def landing(t, j, k):
        if t == 2:
            return r2.at[j, unit(t, k)]
        return r13.at[j, unit(t, k), pl.ds(t * f, f)]

    def send(t, src, j, k, tx, ua, uep):
        return pltpu.make_async_remote_copy(
            src_ref=src, dst_ref=landing(t, j, k), send_sem=tx, recv_sem=rx.at[j, t],
            device_id={"dp": ua, "ep": uep}, device_id_type=pl.DeviceIdType.MESH)

    z, y = lax.div(a, 2), lax.rem(a, 2)

    def tell(sem, dp, ep):
        pl.semaphore_signal(sem, 1, device_id={"dp": dp, "ep": ep}, device_id_type=pl.DeviceIdType.MESH)

    def tell_z(sem):
        @pl.when(z > 0)
        def _():
            tell(sem, a - 2, g)

        @pl.when(z < 3)
        def _():
            tell(sem, a + 2, g)

    nz = _pick((1, 2, 2, 1), z)

    barrier = pltpu.get_barrier_semaphore()
    other = 2 * x + 1 - core
    tell(barrier, a, 2 - 2 * x)
    tell(barrier, a, 3 - 2 * x)
    tell(barrier, a, other)
    tell(barrier, 2 * z + 1 - y, g)
    tell_z(barrier)
    pl.semaphore_wait(barrier, 4 + nz)

    def meet():
        for r in range(2):
            tell_z(ready.at[r])
            pl.semaphore_wait(ready.at[r], nz)
        tell(ready.at[2], 2 * z + 1 - y, g)
        pl.semaphore_wait(ready.at[2], 1)
        tell(ready.at[3], a, other)
        pl.semaphore_wait(ready.at[3], 1)

    for c in range(2):

        @pl.when(core == c)
        def _(c=c):
            width = _pick(HUB[c], a)
            first = _pick(FIRST[c], a)
            slots = SLOTS[c]
            nfwd = _pick(FWD[c], a)
            across = _pick(ACROSS, a)
            nmore = _pick([FWD[c][ACROSS[v]] for v in range(8)], a)
            wacross = _pick([HUB[c][ACROSS[v]] for v in range(8)], a)
            shift = _pick([FIRST[c][ACROSS[v]] - HUB[c][v] for v in range(8)], a)
            low = [_pick([THERE[c][v][s[0]] for v in range(8)], a) for s in slots]
            high = [_pick([THERE[c][v][s[0]] + SERVE[c][v][s[0]] for v in range(8)], a) for s in slots]
            more = [_pick([HUB[c][v] + THERE[c][ACROSS[v]][s[0]] for v in range(8)], a) for s in slots]

            def hunit(i):
                return lax.select(i < width, first, shift) + i

            def forward(i, t):
                return pltpu.make_async_remote_copy(
                    src_ref=raw[t].at[i], dst_ref=raw[t].at[wacross + i], send_sem=f_tx.at[t, i],
                    recv_sem=raw_rx.at[t, wacross + i],
                    device_id={"dp": across, "ep": g}, device_id_type=pl.DeviceIdType.MESH)

            def raw_copy(i, t):
                return pltpu.make_async_remote_copy(
                    src_ref=w[t].at[0, :, unit(t, first + i)], dst_ref=raw[t].at[i],
                    send_sem=raw_tx.at[t, i], recv_sem=raw_rx.at[t, i],
                    device_id={"dp": a, "ep": 2 * (1 - x) + c}, device_id_type=pl.DeviceIdType.MESH)

            def raw_start(i, _):
                for t in range(3):
                    raw_copy(i, t).start()
                return _

            if c == 0:
                lax.fori_loop(0, width, raw_start, 0)
                meet()

                @pl.when(width > 0)
                def _():
                    raw_copy(0, 0).wait_send()

                tell(head, a, g + 1)
            else:
                meet()
                pl.semaphore_wait(head, 1)
                lax.fori_loop(0, width, raw_start, 0)

            dslots = [[(s[1], s[2]) for s in slots if s[0] == u] if NDIR[c][u] else [] for u in range(8)]
            per = max(len(s) for s in dslots)
            count = _pick([max(len(s), 1) for s in dslots], a)
            ndir = _pick(NDIR[c], a)
            nranges = max(len(r) for r in DIRECT[c])
            starts, steps = [], []
            base = _pick([r[0][0] if r else 0 for r in DIRECT[c]], a)
            for q in range(1, nranges):
                starts.append(_pick([sum(hi - lo for lo, hi in r[:q]) if len(r) > q else 999 for r in DIRECT[c]], a))
                steps.append(_pick([r[q][0] - r[q - 1][1] if len(r) > q else 0 for r in DIRECT[c]], a))

            nown = _pick([UNITS if 2 in KIND[u][:2] else 0 for u in range(8)], a) if c == 1 else jnp.int32(0)
            njobs = nown + ndir

            def dunit(n):
                k = base + n
                for st, sp in zip(starts, steps):
                    k = k + lax.select(n >= st, sp, jnp.int32(0))
                return k

            def junit(n):
                return lax.select(n < nown, n, dunit(n - nown)) if c == 1 else dunit(n)

            def load(n, t):
                return pltpu.make_async_copy(w[t].at[0, :, unit(t, junit(n))], dw[t].at[lax.rem(n, 2)], ld.at[t, lax.rem(n, 2)])

            dtab = []
            for q in range(per):
                dtab.append((_pick([len(s) > q for s in dslots], a),
                             _pick([s[q][0] if len(s) > q else 0 for s in dslots], a),
                             _pick([s[q][1] if len(s) > q else 0 for s in dslots], a)))
                dtab[q] += (expert((a * 4 + 2 * (1 - x) + dtab[q][1]) * 2 + dtab[q][2], 2 * x + c),)
            eown = expert((a * 4 + 2 * x) * 2, 2 * x + c)

            def dsend(n, t, q):
                _, uc, j, _ = dtab[q]
                return send(t, ds[t].at[n * count + q], j, dunit(n), d_tx.at[t, n * count + q], a, 2 * (1 - x) + uc)

            def osend(n, t):
                return send(t, os_[t].at[lax.rem(n, ORING)], 0, n, o_tx.at[t, lax.rem(n, ORING)], a, 2 * x)

            @pl.when(njobs > 0)
            def _():
                for t in range(3):
                    load(0, t).start()

            def direct(n):
                for t in range(3):
                    load(n, t).wait()
                    wk[t][...] = dw[t][lax.rem(n, 2)]

                    @pl.when(n + 1 < njobs)
                    def _():
                        load(n + 1, t).start()

                    @pl.when(n >= nown)
                    def _():
                        m = n - nown
                        for q in range(per):
                            @pl.when(dtab[q][0] == 1)
                            def _():
                                e = dtab[q][3]
                                ds[t][m * count + q] = wk[t][e]

                        for q in range(per):

                            @pl.when(dtab[q][0] == 1)
                            def _():
                                dsend(m, t, q).start()

                    if c == 1:

                        @pl.when(n < nown)
                        def _():
                            @pl.when(n >= ORING)
                            def _():
                                osend(n - ORING, t).wait_send()

                            os_[t][lax.rem(n, ORING)] = wk[t][eown]
                            osend(n, t).start()

            picks = [expert((ua * 4 + 2 * x + uc) * 2 + j, 2 * (1 - x) + c) for ua, uc, j in slots]

            def serving(i):
                mine = i < width
                zero = jnp.int32(0)
                return [(i >= lax.select(mine, low[q], zero)) & (i < lax.select(mine, high[q], more[q]))
                        for q in range(len(slots))]

            def hub_do(p, k, t, q, start):
                ua, uc, j = slots[q]
                src, tx = hs[t].at[p, q], h_tx.at[t, p, q]

                def far():
                    cp = send(t, src, j, k, tx, ua, 2 * x + uc)
                    cp.start() if start else cp.wait_send()

                if uc != c:
                    far()
                    return
                pl.when(a != ua)(far)

                @pl.when(a == ua)
                def _():
                    cp = pltpu.make_async_copy(src, landing(t, j, k), tx)
                    cp.start() if start else cp.wait()

            def hub_free(i, on, p, t):
                k = hunit(i)
                for q in range(len(slots)):
                    pl.when(on[q])(functools.partial(hub_do, p, k, t, q, False))

            def hub(i):
                p = lax.rem(i, RING)
                k = hunit(i)
                on = serving(i)
                for t in range(3):

                    @pl.when(i >= RING)
                    def _():
                        hub_free(i - RING, serving(i - RING), p, t)

                    pltpu.make_async_copy(raw[t].at[i], raw[t].at[i], raw_rx.at[t, i]).wait()

                    @pl.when(i < nfwd)
                    def _():
                        forward(i, t).start()

                    wk[t][...] = raw[t][i]
                    for q in range(len(slots)):

                        @pl.when(on[q])
                        def _():
                            hs[t][p, q] = wk[t][picks[q]]

                    for q in range(len(slots)):
                        pl.when(on[q])(functools.partial(hub_do, p, k, t, q, True))

            def loop(lo, hi, f):
                lax.fori_loop(lo, hi, lambda i, s: (f(i), s)[1], 0)

            def raw_drain(i):
                for t in range(3):
                    if c == 0 and t == 0:

                        @pl.when(i > 0)
                        def _():
                            raw_copy(i, 0).wait_send()
                    else:
                        raw_copy(i, t).wait_send()

            most = jnp.maximum(width - 1, 0)
            early = _pick((0, 0, 1, 1, 1, 1, 0, 0), a)

            def drain_most(i):
                @pl.when(i < most)
                def _():
                    raw_drain(i)

            def direct_some(n):
                @pl.when(n < njobs)
                def _():
                    direct(n)

            def mixed(i):
                @pl.when(i == most)
                def _():
                    loop(0, max(HUB[c]) - 1, drain_most)
                    pl.semaphore_signal(clear, 1, device_id={"dp": a, "ep": 2 * x + 1 - c},
                                        device_id_type=pl.DeviceIdType.MESH)
                    if c == 0:

                        @pl.when(early == 1)
                        def _():
                            loop(0, max(NDIR[0]), direct_some)

                def pair(r):
                    @pl.when(i < lax.select(r == 0, width, nmore))
                    def _():
                        hub(i + r * width)

                loop(0, 2, pair)
                if c == 1:

                    @pl.when(i * OWN < nown)
                    def _():
                        loop(0, OWN, lambda r: direct(i * OWN + r))

            ntimes = [max(HUB[c][v], FWD[c][ACROSS[v]], UNITS // OWN if c == 1 and 2 in KIND[v][:2] else 1) for v in range(8)]
            loop(0, _pick(ntimes, a), mixed)

            if c == 0:

                @pl.when(early == 0)
                def _():
                    pl.semaphore_wait(clear, 1)
                    loop(nown, njobs, direct)

                @pl.when(early == 1)
                def _():
                    pl.semaphore_wait(clear, 1)
            else:
                pl.semaphore_wait(clear, 1)
                loop(nown, njobs, direct)
            loop(most, width, raw_drain)

            def forward_drain(i):
                for t in range(3):
                    forward(i, t).wait_send()

            loop(0, nfwd, forward_drain)

            def hub_drain(i, s):
                on = serving(i)
                for t in range(3):
                    hub_free(i, on, lax.rem(i, RING), t)
                return s

            lax.fori_loop(jnp.maximum(width + nmore - RING, 0), width + nmore, hub_drain, 0)

            def direct_drain(n, s):
                for t in range(3):
                    for q in range(per):

                        @pl.when(dtab[q][0] == 1)
                        def _():
                            dsend(n, t, q).wait_send()
                return s

            lax.fori_loop(0, ndir, direct_drain, 0)
            if c == 1:

                def own_drain(n, s):
                    for t in range(3):
                        osend(n, t).wait_send()
                    return s

                lax.fori_loop(jnp.maximum(nown - ORING, 0), nown, own_drain, 0)

            for u in range(8):

                @pl.when(a == u)
                def _(u=u):
                    for j in range(2):
                        kind = KIND[u][2 * c + j]
                        if kind == 3:
                            continue
                        n = UNITS - (SERVE[c][u][u] + THERE[c][ACROSS[u]][u] if kind == c else 0)
                        for t in range(3):
                            if t == 2:
                                part = r2.at[j, pl.ds(0, n * rows[2])]
                            else:
                                part = r13.at[j, pl.ds(0, n * rows[t]), pl.ds(t * f, f)]
                            pltpu.make_async_copy(part, part, rx.at[j, t]).wait()


def _local(nblk, place, wg, wu, wd, r13, r2, o13, o2, buf, lsem, ssem):
    a = lax.axis_index("dp")
    g = lax.axis_index("ep")
    nexp, f = wg.shape[1], wg.shape[3]
    b13 = r13.shape[1] // nblk[0]
    b2 = r2.shape[1] // nblk[1]
    n = 0
    jobs = []
    for j in range(2):
        own = jnp.int32(0)
        for u in range(8):
            for c in range(2):
                if KIND[u][2 * c + j] == 3:
                    own = jnp.where((a == u) & (g % 2 == c), 1, own)
        e = jnp.clip(place[0, (a * 4 + g) * 2 + j] - g * nexp, 0, nexp - 1)
        for b in range(nblk[0] + nblk[1]):
            jobs.append((n, j, b, own, e))
            n += 1
    for n, j, b, own, e in jobs:
        wide = b < nblk[0]
        r = pl.ds(b * b13, b13) if wide else pl.ds((b - nblk[0]) * b2, b2)

        @pl.when(own == 1)
        def _():
            if wide:
                pltpu.make_async_copy(wg.at[0, e, r], buf.at[n, :, pl.ds(0, f)], lsem.at[n]).start()
                pltpu.make_async_copy(wu.at[0, e, r], buf.at[n, :, pl.ds(f, f)], lsem.at[n]).start()
            else:
                pltpu.make_async_copy(wd.at[0, e, r], buf.at[n], lsem.at[n]).start()

        @pl.when(own == 0)
        def _():
            if wide:
                pltpu.make_async_copy(r13.at[j, r], buf.at[n], lsem.at[n]).start()
            else:
                pltpu.make_async_copy(r2.at[j, r], o2.at[0, j, r], ssem.at[n]).start()

    for n, j, b, own, e in jobs:
        wide = b < nblk[0]
        r = pl.ds(b * b13, b13) if wide else pl.ds((b - nblk[0]) * b2, b2)

        def store():
            pltpu.make_async_copy(buf.at[n], buf.at[n], lsem.at[n]).wait()
            pltpu.make_async_copy(buf.at[n], (o13 if wide else o2).at[0, j, r], ssem.at[n]).start()

        store() if wide else pl.when(own == 1)(store)
    for n, j, b, own, e in jobs:
        pltpu.make_async_copy(buf.at[n], buf.at[n], ssem.at[n]).wait()


def solution(mesh):
    anyspec = pl.BlockSpec(memory_space=pl.ANY)
    smem = pl.BlockSpec(memory_space=pltpu.SMEM)

    def body(wg, wu, wd, place):
        _, nexp, d, f = wg.shape
        dt = wg.dtype
        ra, rb = d // UNITS, f // UNITS
        wmax = max(HUB[c][v] + FWD[c][ACROSS[v]] for c in range(2) for v in range(8))
        dma = pltpu.SemaphoreType.DMA

        def three(*lead):
            return [pltpu.VMEM((*lead, ra, f), dt), pltpu.VMEM((*lead, ra, f), dt), pltpu.VMEM((*lead, rb, d), dt)]

        r13, r2 = pl.pallas_call(
            _remote,
            out_shape=(jax.ShapeDtypeStruct((2, d, 2 * f), dt), pltpu.VMEM((2, f, d), dt)),
            in_specs=[smem, anyspec, anyspec, anyspec],
            out_specs=(anyspec, anyspec),
            scratch_shapes=[
                *three(wmax, nexp), *three(2, nexp),
                pltpu.VMEM((nexp, ra, f), dt), pltpu.VMEM((nexp, rb, d), dt),
                *three(RING, MAXS), *three(DSTAGE), *three(ORING),
                dma((3, wmax)), dma((3, wmax)), dma((3, RING, MAXS)), dma((3, DSTAGE)), dma((3, ORING)),
                dma((3, 2)), dma((2, 3)), pltpu.SemaphoreType.REGULAR, pltpu.SemaphoreType.REGULAR, dma((3, wmax)),
                pltpu.SemaphoreType.REGULAR((4,)),
            ],
            compiler_params=pltpu.CompilerParams(has_side_effects=True, collective_id=0, vmem_limit_bytes=52 * 1024 * 1024),
            name="spread",
        )(place, wg, wu, wd)
        r2 = pltpu.with_memory_space_constraint(r2, pltpu.VMEM)
        nblk = (8, 4)
        nbuf = 2 * sum(nblk)
        return pl.pallas_call(
            functools.partial(_local, nblk),
            out_shape=(jax.ShapeDtypeStruct((1, 2, d, 2 * f), dt), jax.ShapeDtypeStruct((1, 2, f, d), dt)),
            in_specs=[smem, anyspec, anyspec, anyspec, anyspec, anyspec],
            out_specs=(anyspec, anyspec),
            scratch_shapes=[pltpu.VMEM((nbuf, d // nblk[0], 2 * f), dt), dma((nbuf,)), dma((nbuf,))],
            compiler_params=pltpu.CompilerParams(vmem_limit_bytes=48 * 1024 * 1024),
            name="settle",
        )(place, wg, wu, wd, r13, r2)

    spec_in = P(None, "ep", None, None)
    spec_out = P(None, ("dp", "ep"), None, None)
    return jax.shard_map(body, mesh=mesh, in_specs=(spec_in, spec_in, spec_in, P(None, None)),
                         out_specs=(spec_out, spec_out), check_vma=False)
```

```python
import functools

import jax
import jax.numpy as jnp
from jax import lax
from jax.experimental import pallas as pl
from jax.experimental.pallas import tpu as pltpu
from jax.sharding import PartitionSpec as P

SUB = 1
UNITS = 32 * SUB
RING = 4 * SUB
ORING = 4
OWN = 8 * SUB
DSTAGE = 22 * SUB

def _rows(*digits):
    return tuple(tuple(SUB * int(d) for d in row) for row in digits)


HUB = _rows("56444405", "00666662")
FWD = _rows("00444400", "00000000")
THERE = (
    _rows("00000000", "00000000", "00004444", "00004434",
          "44440000", "44440000", "00000000", "00000000"),
    _rows(*[8 * "0"] * 8),
)
SERVE = (
    _rows("55532000", "66660600", "44440000", "44440000",
          "00004444", "00004444", "00000000", "00154555"),
    _rows("00000000", "00000000", "66666650", "46666600",
          "20666660", "04666660", "00606660", "00022220"),
)
KIND = []
for _a in range(8):
    _row = []
    for _c in range(2):
        for _j in range(2):
            _g = _c + 2
            _h = (2 * _a - _g) % 4 if _j < ((_a + 1) * 2) // 8 else (_g + _j + 1) % 4
            _row.append(_h if _h < 2 else (3 if _h == _g else 2))
    KIND.append(_row)
SLOTS = tuple(tuple((a, s // 2, s % 2) for a in range(8) for s in range(4) if KIND[a][s] == c) for c in range(2))
ACROSS = tuple(2 * (3 - v // 2) + v % 2 for v in range(8))
FIRST = tuple(tuple(sum(HUB[c][:v]) for v in range(8)) for c in range(2))


def _direct(c, u):
    if not any(s[0] == u for s in SLOTS[c]):
        return []
    out = []
    parts = [(FIRST[c][v] + THERE[c][v][u] + SERVE[c][v][u], FIRST[c][v] + HUB[c][v]) for v in range(8)]
    for lo, hi in parts + [(sum(HUB[c]), UNITS)]:
        if lo == hi:
            continue
        if out and out[-1][1] == lo:
            out[-1][1] = hi
        else:
            out.append([lo, hi])
    return out


BUSY = tuple(tuple([q for q, s in enumerate(SLOTS[c]) if SERVE[c][v][s[0]] or THERE[c][ACROSS[v]][s[0]]] for v in range(8)) for c in range(2))
MAXS = max(len(b) for c in range(2) for b in BUSY[c])
DIRECT = tuple(tuple(_direct(c, u) for u in range(8)) for c in range(2))
NDIR = tuple(tuple(sum(hi - lo for lo, hi in r) for r in DIRECT[c]) for c in range(2))


def _pick(table, i):
    r = jnp.int32(table[0])
    for k in range(1, len(table)):
        if table[k] != table[0]:
            r = lax.select(i == k, jnp.int32(table[k]), r)
    return r


def _remote(place, wg, wu, wd, r13, r2, raw_g, raw_u, raw_d, dw_g, dw_u, dw_d, wk13, wk2, hs_g, hs_u, hs_d,
            ds_g, ds_u, ds_d, os_g, os_u, os_d, raw_rx, raw_tx, h_tx, d_tx, o_tx, ld, rx, clear, head, f_tx, ready):
    a = lax.axis_index("dp")
    g = lax.axis_index("ep")
    x = lax.div(g, 2)
    core = lax.rem(g, 2)
    w, raw, dw = (wg, wu, wd), (raw_g, raw_u, raw_d), (dw_g, dw_u, dw_d)
    hs, ds, os_, wk = (hs_g, hs_u, hs_d), (ds_g, ds_u, ds_d), (os_g, os_u, os_d), (wk13, wk13, wk2)
    nexp, f = wg.shape[1], wg.shape[3]
    rows = tuple(r.shape[2] for r in raw)

    def expert(s, h):
        return jnp.clip(place[0, s] - h * nexp, 0, nexp - 1)

    def unit(t, k):
        return pl.ds(pl.multiple_of(k * rows[t], rows[t]), rows[t])

    def landing(t, j, k):
        if t == 2:
            return r2.at[j, unit(t, k)]
        return r13.at[j, unit(t, k), pl.ds(t * f, f)]

    def send(t, src, j, k, tx, ua, uep):
        return pltpu.make_async_remote_copy(
            src_ref=src, dst_ref=landing(t, j, k), send_sem=tx, recv_sem=rx.at[j, t],
            device_id={"dp": ua, "ep": uep}, device_id_type=pl.DeviceIdType.MESH)

    z, y = lax.div(a, 2), lax.rem(a, 2)

    def tell(sem, dp, ep):
        pl.semaphore_signal(sem, 1, device_id={"dp": dp, "ep": ep}, device_id_type=pl.DeviceIdType.MESH)

    def tell_z(sem):
        @pl.when(z > 0)
        def _():
            tell(sem, a - 2, g)

        @pl.when(z < 3)
        def _():
            tell(sem, a + 2, g)

    nz = _pick((1, 2, 2, 1), z)

    barrier = pltpu.get_barrier_semaphore()
    other = 2 * x + 1 - core
    tell(barrier, a, 2 - 2 * x)
    tell(barrier, a, 3 - 2 * x)
    tell(barrier, a, other)
    tell(barrier, 2 * z + 1 - y, g)
    tell_z(barrier)
    pl.semaphore_wait(barrier, 4 + nz)

    def meet():
        for r in range(2):
            tell_z(ready.at[r])
            pl.semaphore_wait(ready.at[r], nz)
        tell(ready.at[2], 2 * z + 1 - y, g)
        pl.semaphore_wait(ready.at[2], 1)
        tell(ready.at[3], a, other)
        pl.semaphore_wait(ready.at[3], 1)

    for c in range(2):

        @pl.when(core == c)
        def _(c=c):
            width = _pick(HUB[c], a)
            first = _pick(FIRST[c], a)
            slots = SLOTS[c]
            nfwd = _pick(FWD[c], a)
            across = _pick(ACROSS, a)
            nmore = _pick([FWD[c][ACROSS[v]] for v in range(8)], a)
            wacross = _pick([HUB[c][ACROSS[v]] for v in range(8)], a)
            shift = _pick([FIRST[c][ACROSS[v]] - HUB[c][v] for v in range(8)], a)
            low = [_pick([THERE[c][v][s[0]] for v in range(8)], a) for s in slots]
            high = [_pick([THERE[c][v][s[0]] + SERVE[c][v][s[0]] for v in range(8)], a) for s in slots]
            more = [_pick([HUB[c][v] + THERE[c][ACROSS[v]][s[0]] for v in range(8)], a) for s in slots]

            def hunit(i):
                return lax.select(i < width, first, shift) + i

            def forward(i, t):
                return pltpu.make_async_remote_copy(
                    src_ref=raw[t].at[i], dst_ref=raw[t].at[wacross + i], send_sem=f_tx.at[t, i],
                    recv_sem=raw_rx.at[t, wacross + i],
                    device_id={"dp": across, "ep": g}, device_id_type=pl.DeviceIdType.MESH)

            def raw_copy(i, t):
                return pltpu.make_async_remote_copy(
                    src_ref=w[t].at[0, :, unit(t, first + i)], dst_ref=raw[t].at[i],
                    send_sem=raw_tx.at[t, i], recv_sem=raw_rx.at[t, i],
                    device_id={"dp": a, "ep": 2 * (1 - x) + c}, device_id_type=pl.DeviceIdType.MESH)

            def raw_start(i, _):
                for t in range(3):
                    raw_copy(i, t).start()
                return _

            if c == 0:
                lax.fori_loop(0, width, raw_start, 0)
                meet()

                @pl.when(width > 0)
                def _():
                    raw_copy(0, 0).wait_send()

                tell(head, a, g + 1)
            else:
                meet()
                pl.semaphore_wait(head, 1)
                lax.fori_loop(0, width, raw_start, 0)

            dslots = [[(s[1], s[2]) for s in slots if s[0] == u] if NDIR[c][u] else [] for u in range(8)]
            per = max(len(s) for s in dslots)
            count = _pick([max(len(s), 1) for s in dslots], a)
            ndir = _pick(NDIR[c], a)
            nranges = max(len(r) for r in DIRECT[c])
            starts, steps = [], []
            base = _pick([r[0][0] if r else 0 for r in DIRECT[c]], a)
            for q in range(1, nranges):
                starts.append(_pick([sum(hi - lo for lo, hi in r[:q]) if len(r) > q else 999 for r in DIRECT[c]], a))
                steps.append(_pick([r[q][0] - r[q - 1][1] if len(r) > q else 0 for r in DIRECT[c]], a))

            nown = _pick([UNITS if 2 in KIND[u][:2] else 0 for u in range(8)], a) if c == 1 else jnp.int32(0)
            njobs = nown + ndir

            def dunit(n):
                k = base + n
                for st, sp in zip(starts, steps):
                    k = k + lax.select(n >= st, sp, jnp.int32(0))
                return k

            def junit(n):
                return lax.select(n < nown, n, dunit(n - nown)) if c == 1 else dunit(n)

            def load(n, t):
                return pltpu.make_async_copy(w[t].at[0, :, unit(t, junit(n))], dw[t].at[lax.rem(n, 2)], ld.at[t, lax.rem(n, 2)])

            dtab = []
            for q in range(per):
                dtab.append((_pick([len(s) > q for s in dslots], a),
                             _pick([s[q][0] if len(s) > q else 0 for s in dslots], a),
                             _pick([s[q][1] if len(s) > q else 0 for s in dslots], a)))
                dtab[q] += (expert((a * 4 + 2 * (1 - x) + dtab[q][1]) * 2 + dtab[q][2], 2 * x + c),)
            eown = expert((a * 4 + 2 * x) * 2, 2 * x + c)

            def dsend(n, t, q):
                _, uc, j, _ = dtab[q]
                return send(t, ds[t].at[n * count + q], j, dunit(n), d_tx.at[t, n * count + q], a, 2 * (1 - x) + uc)

            def osend(n, t):
                return send(t, os_[t].at[lax.rem(n, ORING)], 0, n, o_tx.at[t, lax.rem(n, ORING)], a, 2 * x)

            @pl.when(njobs > 0)
            def _():
                for t in range(3):
                    load(0, t).start()

            def direct(n):
                for t in range(3):
                    load(n, t).wait()
                    wk[t][...] = dw[t][lax.rem(n, 2)]

                    @pl.when(n + 1 < njobs)
                    def _():
                        load(n + 1, t).start()

                    @pl.when(n >= nown)
                    def _():
                        m = n - nown
                        for q in range(per):
                            @pl.when(dtab[q][0] == 1)
                            def _():
                                e = dtab[q][3]
                                ds[t][m * count + q] = wk[t][e]

                        for q in range(per):

                            @pl.when(dtab[q][0] == 1)
                            def _():
                                dsend(m, t, q).start()

                    if c == 1:

                        @pl.when(n < nown)
                        def _():
                            @pl.when(n >= ORING)
                            def _():
                                osend(n - ORING, t).wait_send()

                            os_[t][lax.rem(n, ORING)] = wk[t][eown]
                            osend(n, t).start()

            picks = [expert((ua * 4 + 2 * x + uc) * 2 + j, 2 * (1 - x) + c) for ua, uc, j in slots]

            spot = [_pick([b.index(q) if q in b else 0 for b in BUSY[c]], a) for q in range(len(slots))]

            def serving(i):
                mine = i < width
                zero = jnp.int32(0)
                return [(i >= lax.select(mine, low[q], zero)) & (i < lax.select(mine, high[q], more[q]))
                        for q in range(len(slots))]

            def hub_do(p, k, t, q, start):
                ua, uc, j = slots[q]
                src, tx = hs[t].at[p, spot[q]], h_tx.at[t, p, spot[q]]

                def far():
                    cp = send(t, src, j, k, tx, ua, 2 * x + uc)
                    cp.start() if start else cp.wait_send()

                if uc != c:
                    far()
                    return
                pl.when(a != ua)(far)

                @pl.when(a == ua)
                def _():
                    cp = pltpu.make_async_copy(src, landing(t, j, k), tx)
                    cp.start() if start else cp.wait()

            def hub_free(i, on, p, t):
                k = hunit(i)
                for q in range(len(slots)):
                    pl.when(on[q])(functools.partial(hub_do, p, k, t, q, False))

            def hub(i):
                p = lax.rem(i, RING)
                k = hunit(i)
                on = serving(i)
                for t in range(3):

                    @pl.when(i >= RING)
                    def _():
                        hub_free(i - RING, serving(i - RING), p, t)

                    pltpu.make_async_copy(raw[t].at[i], raw[t].at[i], raw_rx.at[t, i]).wait()

                    @pl.when(i < nfwd)
                    def _():
                        forward(i, t).start()

                    wk[t][...] = raw[t][i]
                    for q in range(len(slots)):

                        @pl.when(on[q])
                        def _():
                            hs[t][p, spot[q]] = wk[t][picks[q]]

                    for q in range(len(slots)):
                        pl.when(on[q])(functools.partial(hub_do, p, k, t, q, True))

            def loop(lo, hi, f):
                lax.fori_loop(lo, hi, lambda i, s: (f(i), s)[1], 0)

            def raw_drain(i):
                for t in range(3):
                    if c == 0 and t == 0:

                        @pl.when(i > 0)
                        def _():
                            raw_copy(i, 0).wait_send()
                    else:
                        raw_copy(i, t).wait_send()

            most = jnp.maximum(width - 1, 0)
            early = _pick((0, 0, 1, 1, 1, 1, 0, 0), a)

            def drain_most(i):
                @pl.when(i < most)
                def _():
                    raw_drain(i)

            def direct_some(n):
                @pl.when(n < njobs)
                def _():
                    direct(n)

            def mixed(i):
                @pl.when(i == most)
                def _():
                    loop(0, max(HUB[c]) - 1, drain_most)
                    pl.semaphore_signal(clear, 1, device_id={"dp": a, "ep": 2 * x + 1 - c},
                                        device_id_type=pl.DeviceIdType.MESH)
                    if c == 0:

                        @pl.when(early == 1)
                        def _():
                            loop(0, max(NDIR[0]), direct_some)

                def pair(r):
                    @pl.when(i < lax.select(r == 0, width, nmore))
                    def _():
                        hub(i + r * width)

                loop(0, 2, pair)
                if c == 1:

                    @pl.when(i * OWN < nown)
                    def _():
                        loop(0, OWN, lambda r: direct(i * OWN + r))

            ntimes = [max(HUB[c][v], FWD[c][ACROSS[v]], UNITS // OWN if c == 1 and 2 in KIND[v][:2] else 1) for v in range(8)]
            loop(0, _pick(ntimes, a), mixed)

            if c == 0:

                @pl.when(early == 0)
                def _():
                    pl.semaphore_wait(clear, 1)
                    loop(nown, njobs, direct)

                @pl.when(early == 1)
                def _():
                    pl.semaphore_wait(clear, 1)
            else:
                pl.semaphore_wait(clear, 1)
                loop(nown, njobs, direct)
            loop(most, width, raw_drain)

            def forward_drain(i):
                for t in range(3):
                    forward(i, t).wait_send()

            loop(0, nfwd, forward_drain)

            def hub_drain(i, s):
                on = serving(i)
                for t in range(3):
                    hub_free(i, on, lax.rem(i, RING), t)
                return s

            lax.fori_loop(jnp.maximum(width + nmore - RING, 0), width + nmore, hub_drain, 0)

            def direct_drain(n, s):
                for t in range(3):
                    for q in range(per):

                        @pl.when(dtab[q][0] == 1)
                        def _():
                            dsend(n, t, q).wait_send()
                return s

            lax.fori_loop(0, ndir, direct_drain, 0)
            if c == 1:

                def own_drain(n, s):
                    for t in range(3):
                        osend(n, t).wait_send()
                    return s

                lax.fori_loop(jnp.maximum(nown - ORING, 0), nown, own_drain, 0)

            for u in range(8):

                @pl.when(a == u)
                def _(u=u):
                    for j in range(2):
                        kind = KIND[u][2 * c + j]
                        if kind == 3:
                            continue
                        n = UNITS - (SERVE[c][u][u] + THERE[c][ACROSS[u]][u] if kind == c else 0)
                        for t in range(3):
                            if t == 2:
                                part = r2.at[j, pl.ds(0, n * rows[2])]
                            else:
                                part = r13.at[j, pl.ds(0, n * rows[t]), pl.ds(t * f, f)]
                            pltpu.make_async_copy(part, part, rx.at[j, t]).wait()


def _local(nblk, place, wg, wu, wd, r13, r2, o13, o2, buf, lsem, ssem):
    a = lax.axis_index("dp")
    g = lax.axis_index("ep")
    nexp, f = wg.shape[1], wg.shape[3]
    b13 = r13.shape[1] // nblk[0]
    b2 = r2.shape[1] // nblk[1]
    n = 0
    jobs = []
    for j in range(2):
        own = jnp.int32(0)
        for u in range(8):
            for c in range(2):
                if KIND[u][2 * c + j] == 3:
                    own = jnp.where((a == u) & (g % 2 == c), 1, own)
        e = jnp.clip(place[0, (a * 4 + g) * 2 + j] - g * nexp, 0, nexp - 1)
        for b in range(nblk[0] + nblk[1]):
            jobs.append((n, j, b, own, e))
            n += 1
    for n, j, b, own, e in jobs:
        wide = b < nblk[0]
        r = pl.ds(b * b13, b13) if wide else pl.ds((b - nblk[0]) * b2, b2)

        @pl.when(own == 1)
        def _():
            if wide:
                pltpu.make_async_copy(wg.at[0, e, r], buf.at[n, :, pl.ds(0, f)], lsem.at[n]).start()
                pltpu.make_async_copy(wu.at[0, e, r], buf.at[n, :, pl.ds(f, f)], lsem.at[n]).start()
            else:
                pltpu.make_async_copy(wd.at[0, e, r], buf.at[n], lsem.at[n]).start()

        @pl.when(own == 0)
        def _():
            if wide:
                pltpu.make_async_copy(r13.at[j, r], o13.at[0, j, r], ssem.at[n]).start()
            else:
                pltpu.make_async_copy(r2.at[j, r], buf.at[n], lsem.at[n]).start()

    for n, j, b, own, e in jobs:
        wide = b < nblk[0]
        r = pl.ds(b * b13, b13) if wide else pl.ds((b - nblk[0]) * b2, b2)

        def store():
            pltpu.make_async_copy(buf.at[n], buf.at[n], lsem.at[n]).wait()
            pltpu.make_async_copy(buf.at[n], (o13 if wide else o2).at[0, j, r], ssem.at[n]).start()

        pl.when(own == 1)(store) if wide else store()
    for n, j, b, own, e in jobs:
        pltpu.make_async_copy(buf.at[n], buf.at[n], ssem.at[n]).wait()


def solution(mesh):
    anyspec = pl.BlockSpec(memory_space=pl.ANY)
    smem = pl.BlockSpec(memory_space=pltpu.SMEM)

    def body(wg, wu, wd, place):
        _, nexp, d, f = wg.shape
        dt = wg.dtype
        ra, rb = d // UNITS, f // UNITS
        wmax = max(HUB[c][v] + FWD[c][ACROSS[v]] for c in range(2) for v in range(8))
        dma = pltpu.SemaphoreType.DMA

        def three(*lead):
            return [pltpu.VMEM((*lead, ra, f), dt), pltpu.VMEM((*lead, ra, f), dt), pltpu.VMEM((*lead, rb, d), dt)]

        r13, r2 = pl.pallas_call(
            _remote,
            out_shape=(pltpu.VMEM((2, d, 2 * f), dt), jax.ShapeDtypeStruct((2, f, d), dt)),
            in_specs=[smem, anyspec, anyspec, anyspec],
            out_specs=(anyspec, anyspec),
            scratch_shapes=[
                *three(wmax, nexp), *three(2, nexp),
                pltpu.VMEM((nexp, ra, f), dt), pltpu.VMEM((nexp, rb, d), dt),
                *three(RING, MAXS), *three(DSTAGE), *three(ORING),
                dma((3, wmax)), dma((3, wmax)), dma((3, RING, MAXS)), dma((3, DSTAGE)), dma((3, ORING)),
                dma((3, 2)), dma((2, 3)), pltpu.SemaphoreType.REGULAR, pltpu.SemaphoreType.REGULAR, dma((3, wmax)),
                pltpu.SemaphoreType.REGULAR((4,)),
            ],
            compiler_params=pltpu.CompilerParams(has_side_effects=True, collective_id=0, vmem_limit_bytes=46 * 1024 * 1024),
            name="spread",
        )(place, wg, wu, wd)
        r13 = pltpu.with_memory_space_constraint(r13, pltpu.VMEM)
        nblk = (8, 4)
        nbuf = 2 * sum(nblk)
        return pl.pallas_call(
            functools.partial(_local, nblk),
            out_shape=(jax.ShapeDtypeStruct((1, 2, d, 2 * f), dt), jax.ShapeDtypeStruct((1, 2, f, d), dt)),
            in_specs=[smem, anyspec, anyspec, anyspec, anyspec, anyspec],
            out_specs=(anyspec, anyspec),
            scratch_shapes=[pltpu.VMEM((nbuf, d // nblk[0], 2 * f), dt), dma((nbuf,)), dma((nbuf,))],
            compiler_params=pltpu.CompilerParams(vmem_limit_bytes=44 * 1024 * 1024),
            name="settle",
        )(place, wg, wu, wd, r13, r2)

    spec_in = P(None, "ep", None, None)
    spec_out = P(None, ("dp", "ep"), None, None)
    return jax.shard_map(body, mesh=mesh, in_specs=(spec_in, spec_in, spec_in, P(None, None)),
                         out_specs=(spec_out, spec_out), check_vma=False)
```

```python
import functools

import jax
import jax.numpy as jnp
from jax import lax
from jax.experimental import pallas as pl
from jax.experimental.pallas import tpu as pltpu
from jax.sharding import PartitionSpec as P

SUB = 1
UNITS = 32 * SUB
RING = 4 * SUB
ORING = 2
OWN = 8 * SUB
DSTAGE = 22 * SUB

def _rows(*digits):
    return tuple(tuple(SUB * int(d) for d in row) for row in digits)


HUB = _rows("56444405", "00666662")
FWD = _rows("00444400", "00000000")
THERE = (
    _rows("00000000", "00000000", "00004444", "00004434",
          "44440000", "44440000", "00000000", "00000000"),
    _rows(*[8 * "0"] * 8),
)
SERVE = (
    _rows("55532000", "66660600", "44440000", "44440000",
          "00004444", "00004444", "00000000", "00154555"),
    _rows("00000000", "00000000", "66666650", "46666600",
          "20666660", "04666660", "00606660", "00022220"),
)
KIND = []
for _a in range(8):
    _row = []
    for _c in range(2):
        for _j in range(2):
            _g = _c + 2
            _h = (2 * _a - _g) % 4 if _j < ((_a + 1) * 2) // 8 else (_g + _j + 1) % 4
            _row.append(_h if _h < 2 else (3 if _h == _g else 2))
    KIND.append(_row)
SLOTS = tuple(tuple((a, s // 2, s % 2) for a in range(8) for s in range(4) if KIND[a][s] == c) for c in range(2))
ACROSS = tuple(2 * (3 - v // 2) + v % 2 for v in range(8))
FIRST = tuple(tuple(sum(HUB[c][:v]) for v in range(8)) for c in range(2))


def _direct(c, u):
    if not any(s[0] == u for s in SLOTS[c]):
        return []
    out = []
    parts = [(FIRST[c][v] + THERE[c][v][u] + SERVE[c][v][u], FIRST[c][v] + HUB[c][v]) for v in range(8)]
    for lo, hi in parts + [(sum(HUB[c]), UNITS)]:
        if lo == hi:
            continue
        if out and out[-1][1] == lo:
            out[-1][1] = hi
        else:
            out.append([lo, hi])
    return out


BUSY = tuple(tuple([q for q, s in enumerate(SLOTS[c]) if SERVE[c][v][s[0]] or THERE[c][ACROSS[v]][s[0]]] for v in range(8)) for c in range(2))
MAXS = max(len(b) for c in range(2) for b in BUSY[c])
DIRECT = tuple(tuple(_direct(c, u) for u in range(8)) for c in range(2))
NDIR = tuple(tuple(sum(hi - lo for lo, hi in r) for r in DIRECT[c]) for c in range(2))


def _pick(table, i):
    r = jnp.int32(table[0])
    for k in range(1, len(table)):
        if table[k] != table[0]:
            r = lax.select(i == k, jnp.int32(table[k]), r)
    return r


def _remote(place, wg, wu, wd, r13, r2, raw_g, raw_u, raw_d, dw_g, dw_u, dw_d, wk13, wk2, hs_g, hs_u, hs_d,
            ds_g, ds_u, ds_d, os_g, os_u, os_d, raw_rx, raw_tx, h_tx, d_tx, o_tx, ld, rx, clear, head, f_tx, ready):
    a = lax.axis_index("dp")
    g = lax.axis_index("ep")
    x = lax.div(g, 2)
    core = lax.rem(g, 2)
    w, raw, dw = (wg, wu, wd), (raw_g, raw_u, raw_d), (dw_g, dw_u, dw_d)
    hs, ds, os_, wk = (hs_g, hs_u, hs_d), (ds_g, ds_u, ds_d), (os_g, os_u, os_d), (wk13, wk13, wk2)
    nexp, f = wg.shape[1], wg.shape[3]
    rows = tuple(r.shape[2] for r in raw)

    def expert(s, h):
        return jnp.clip(place[0, s] - h * nexp, 0, nexp - 1)

    def unit(t, k):
        return pl.ds(pl.multiple_of(k * rows[t], rows[t]), rows[t])

    def landing(t, j, k):
        if t == 2:
            return r2.at[j, unit(t, k)]
        return r13.at[j, unit(t, k), pl.ds(t * f, f)]

    def send(t, src, j, k, tx, ua, uep):
        return pltpu.make_async_remote_copy(
            src_ref=src, dst_ref=landing(t, j, k), send_sem=tx, recv_sem=rx.at[j, t],
            device_id={"dp": ua, "ep": uep}, device_id_type=pl.DeviceIdType.MESH)

    z, y = lax.div(a, 2), lax.rem(a, 2)

    def tell(sem, dp, ep):
        pl.semaphore_signal(sem, 1, device_id={"dp": dp, "ep": ep}, device_id_type=pl.DeviceIdType.MESH)

    def tell_z(sem):
        @pl.when(z > 0)
        def _():
            tell(sem, a - 2, g)

        @pl.when(z < 3)
        def _():
            tell(sem, a + 2, g)

    nz = _pick((1, 2, 2, 1), z)

    barrier = pltpu.get_barrier_semaphore()
    other = 2 * x + 1 - core
    tell(barrier, a, 2 - 2 * x)
    tell(barrier, a, 3 - 2 * x)
    tell(barrier, a, other)
    tell(barrier, 2 * z + 1 - y, g)
    tell_z(barrier)
    pl.semaphore_wait(barrier, 4 + nz)

    def meet():
        for r in range(2):
            tell_z(ready.at[r])
            pl.semaphore_wait(ready.at[r], nz)
        tell(ready.at[2], 2 * z + 1 - y, g)
        pl.semaphore_wait(ready.at[2], 1)
        tell(ready.at[3], a, other)
        pl.semaphore_wait(ready.at[3], 1)

    for c in range(2):

        @pl.when(core == c)
        def _(c=c):
            width = _pick(HUB[c], a)
            first = _pick(FIRST[c], a)
            slots = SLOTS[c]
            nfwd = _pick(FWD[c], a)
            across = _pick(ACROSS, a)
            nmore = _pick([FWD[c][ACROSS[v]] for v in range(8)], a)
            wacross = _pick([HUB[c][ACROSS[v]] for v in range(8)], a)
            shift = _pick([FIRST[c][ACROSS[v]] - HUB[c][v] for v in range(8)], a)
            low = [_pick([THERE[c][v][s[0]] for v in range(8)], a) for s in slots]
            high = [_pick([THERE[c][v][s[0]] + SERVE[c][v][s[0]] for v in range(8)], a) for s in slots]
            more = [_pick([HUB[c][v] + THERE[c][ACROSS[v]][s[0]] for v in range(8)], a) for s in slots]

            def hunit(i):
                return lax.select(i < width, first, shift) + i

            def forward(i, t):
                return pltpu.make_async_remote_copy(
                    src_ref=raw[t].at[i], dst_ref=raw[t].at[wacross + i], send_sem=f_tx.at[t, i],
                    recv_sem=raw_rx.at[t, wacross + i],
                    device_id={"dp": across, "ep": g}, device_id_type=pl.DeviceIdType.MESH)

            def raw_copy(i, t):
                return pltpu.make_async_remote_copy(
                    src_ref=w[t].at[0, :, unit(t, first + i)], dst_ref=raw[t].at[i],
                    send_sem=raw_tx.at[t, i], recv_sem=raw_rx.at[t, i],
                    device_id={"dp": a, "ep": 2 * (1 - x) + c}, device_id_type=pl.DeviceIdType.MESH)

            def raw_start(i, _):
                for t in range(3):
                    raw_copy(i, t).start()
                return _

            if c == 0:
                lax.fori_loop(0, width, raw_start, 0)
                meet()

                @pl.when(width > 0)
                def _():
                    raw_copy(0, 0).wait_send()

                tell(head, a, g + 1)
            else:
                meet()
                pl.semaphore_wait(head, 1)
                lax.fori_loop(0, width, raw_start, 0)

            dslots = [[(s[1], s[2]) for s in slots if s[0] == u] if NDIR[c][u] else [] for u in range(8)]
            per = max(len(s) for s in dslots)
            count = _pick([max(len(s), 1) for s in dslots], a)
            ndir = _pick(NDIR[c], a)
            nranges = max(len(r) for r in DIRECT[c])
            starts, steps = [], []
            base = _pick([r[0][0] if r else 0 for r in DIRECT[c]], a)
            for q in range(1, nranges):
                starts.append(_pick([sum(hi - lo for lo, hi in r[:q]) if len(r) > q else 999 for r in DIRECT[c]], a))
                steps.append(_pick([r[q][0] - r[q - 1][1] if len(r) > q else 0 for r in DIRECT[c]], a))

            nown = _pick([UNITS if 2 in KIND[u][:2] else 0 for u in range(8)], a) if c == 1 else jnp.int32(0)
            njobs = nown + ndir

            def dunit(n):
                k = base + n
                for st, sp in zip(starts, steps):
                    k = k + lax.select(n >= st, sp, jnp.int32(0))
                return k

            def junit(n):
                return lax.select(n < nown, n, dunit(n - nown)) if c == 1 else dunit(n)

            def load(n, t):
                return pltpu.make_async_copy(w[t].at[0, :, unit(t, junit(n))], dw[t], ld.at[t])

            dtab = []
            for q in range(per):
                dtab.append((_pick([len(s) > q for s in dslots], a),
                             _pick([s[q][0] if len(s) > q else 0 for s in dslots], a),
                             _pick([s[q][1] if len(s) > q else 0 for s in dslots], a)))
                dtab[q] += (expert((a * 4 + 2 * (1 - x) + dtab[q][1]) * 2 + dtab[q][2], 2 * x + c),)
            eown = expert((a * 4 + 2 * x) * 2, 2 * x + c)

            def dsend(n, t, q):
                _, uc, j, _ = dtab[q]
                return send(t, ds[t].at[n * count + q], j, dunit(n), d_tx.at[t, n * count + q], a, 2 * (1 - x) + uc)

            def osend(n, t):
                return send(t, os_[t].at[lax.rem(n, ORING)], 0, n, o_tx.at[t, lax.rem(n, ORING)], a, 2 * x)

            @pl.when(njobs > 0)
            def _():
                for t in range(3):
                    load(0, t).start()

            def direct(n):
                for t in range(3):
                    load(n, t).wait()
                    wk[t][...] = dw[t][...]

                    @pl.when(n + 1 < njobs)
                    def _():
                        load(n + 1, t).start()

                    @pl.when(n >= nown)
                    def _():
                        m = n - nown
                        for q in range(per):
                            @pl.when(dtab[q][0] == 1)
                            def _():
                                e = dtab[q][3]
                                ds[t][m * count + q] = wk[t][e]

                        for q in range(per):

                            @pl.when(dtab[q][0] == 1)
                            def _():
                                dsend(m, t, q).start()

                    if c == 1:

                        @pl.when(n < nown)
                        def _():
                            @pl.when(n >= ORING)
                            def _():
                                osend(n - ORING, t).wait_send()

                            os_[t][lax.rem(n, ORING)] = wk[t][eown]
                            osend(n, t).start()

            picks = [expert((ua * 4 + 2 * x + uc) * 2 + j, 2 * (1 - x) + c) for ua, uc, j in slots]

            spot = [_pick([b.index(q) if q in b else 0 for b in BUSY[c]], a) for q in range(len(slots))]

            def serving(i):
                mine = i < width
                zero = jnp.int32(0)
                return [(i >= lax.select(mine, low[q], zero)) & (i < lax.select(mine, high[q], more[q]))
                        for q in range(len(slots))]

            def hub_do(p, k, t, q, start):
                ua, uc, j = slots[q]
                src, tx = hs[t].at[p, spot[q]], h_tx.at[t, p, spot[q]]

                def far():
                    cp = send(t, src, j, k, tx, ua, 2 * x + uc)
                    cp.start() if start else cp.wait_send()

                if uc != c:
                    far()
                    return
                pl.when(a != ua)(far)

                @pl.when(a == ua)
                def _():
                    cp = pltpu.make_async_copy(src, landing(t, j, k), tx)
                    cp.start() if start else cp.wait()

            def hub_free(i, on, p, t):
                k = hunit(i)
                for q in range(len(slots)):
                    pl.when(on[q])(functools.partial(hub_do, p, k, t, q, False))

            def hub(i):
                p = lax.rem(i, RING)
                k = hunit(i)
                on = serving(i)
                for t in range(3):

                    @pl.when(i >= RING)
                    def _():
                        hub_free(i - RING, serving(i - RING), p, t)

                    pltpu.make_async_copy(raw[t].at[i], raw[t].at[i], raw_rx.at[t, i]).wait()

                    @pl.when(i < nfwd)
                    def _():
                        forward(i, t).start()

                    wk[t][...] = raw[t][i]
                    for q in range(len(slots)):

                        @pl.when(on[q])
                        def _():
                            hs[t][p, spot[q]] = wk[t][picks[q]]

                    for q in range(len(slots)):
                        pl.when(on[q])(functools.partial(hub_do, p, k, t, q, True))

            def loop(lo, hi, f):
                lax.fori_loop(lo, hi, lambda i, s: (f(i), s)[1], 0)

            def raw_drain(i):
                for t in range(3):
                    if c == 0 and t == 0:

                        @pl.when(i > 0)
                        def _():
                            raw_copy(i, 0).wait_send()
                    else:
                        raw_copy(i, t).wait_send()

            most = jnp.maximum(width - 1, 0)
            early = _pick((0, 0, 1, 1, 1, 1, 0, 0), a)

            def drain_most(i):
                @pl.when(i < most)
                def _():
                    raw_drain(i)

            def direct_some(n):
                @pl.when(n < njobs)
                def _():
                    direct(n)

            def mixed(i):
                @pl.when(i == most)
                def _():
                    loop(0, max(HUB[c]) - 1, drain_most)
                    pl.semaphore_signal(clear, 1, device_id={"dp": a, "ep": 2 * x + 1 - c},
                                        device_id_type=pl.DeviceIdType.MESH)
                    if c == 0:

                        @pl.when(early == 1)
                        def _():
                            loop(0, max(NDIR[0]), direct_some)

                def pair(r):
                    @pl.when(i < lax.select(r == 0, width, nmore))
                    def _():
                        hub(i + r * width)

                loop(0, 2, pair)
                if c == 1:

                    @pl.when(i * OWN < nown)
                    def _():
                        loop(0, OWN, lambda r: direct(i * OWN + r))

            ntimes = [max(HUB[c][v], FWD[c][ACROSS[v]], UNITS // OWN if c == 1 and 2 in KIND[v][:2] else 1) for v in range(8)]
            loop(0, _pick(ntimes, a), mixed)

            if c == 0:

                @pl.when(early == 0)
                def _():
                    pl.semaphore_wait(clear, 1)
                    loop(nown, njobs, direct)

                @pl.when(early == 1)
                def _():
                    pl.semaphore_wait(clear, 1)
            else:
                pl.semaphore_wait(clear, 1)
                loop(nown, njobs, direct)
            loop(most, width, raw_drain)

            def forward_drain(i):
                for t in range(3):
                    forward(i, t).wait_send()

            loop(0, nfwd, forward_drain)

            def hub_drain(i, s):
                on = serving(i)
                for t in range(3):
                    hub_free(i, on, lax.rem(i, RING), t)
                return s

            lax.fori_loop(jnp.maximum(width + nmore - RING, 0), width + nmore, hub_drain, 0)

            def direct_drain(n, s):
                for t in range(3):
                    for q in range(per):

                        @pl.when(dtab[q][0] == 1)
                        def _():
                            dsend(n, t, q).wait_send()
                return s

            lax.fori_loop(0, ndir, direct_drain, 0)
            if c == 1:

                def own_drain(n, s):
                    for t in range(3):
                        osend(n, t).wait_send()
                    return s

                lax.fori_loop(jnp.maximum(nown - ORING, 0), nown, own_drain, 0)

            for u in range(8):

                @pl.when(a == u)
                def _(u=u):
                    for j in range(2):
                        kind = KIND[u][2 * c + j]
                        if kind == 3:
                            continue
                        n = UNITS - (SERVE[c][u][u] + THERE[c][ACROSS[u]][u] if kind == c else 0)
                        for t in range(3):
                            if t == 2:
                                part = r2.at[j, pl.ds(0, n * rows[2])]
                            else:
                                part = r13.at[j, pl.ds(0, n * rows[t]), pl.ds(t * f, f)]
                            pltpu.make_async_copy(part, part, rx.at[j, t]).wait()


def _local(nblk, place, wg, wu, wd, r13, r2, o13, o2, buf, lsem, ssem):
    a = lax.axis_index("dp")
    g = lax.axis_index("ep")
    nexp, f = wg.shape[1], wg.shape[3]
    b13 = r13.shape[1] // nblk[0]
    b2 = r2.shape[1] // nblk[1]
    n = 0
    jobs = []
    for j in range(2):
        own = jnp.int32(0)
        for u in range(8):
            for c in range(2):
                if KIND[u][2 * c + j] == 3:
                    own = jnp.where((a == u) & (g % 2 == c), 1, own)
        e = jnp.clip(place[0, (a * 4 + g) * 2 + j] - g * nexp, 0, nexp - 1)
        for b in range(nblk[0] + nblk[1]):
            jobs.append((n, j, b, own, e))
            n += 1
    for n, j, b, own, e in jobs:
        wide = b < nblk[0]
        r = pl.ds(b * b13, b13) if wide else pl.ds((b - nblk[0]) * b2, b2)

        @pl.when(own == 1)
        def _():
            if wide:
                pltpu.make_async_copy(wg.at[0, e, r], buf.at[n, :, pl.ds(0, f)], lsem.at[n]).start()
                pltpu.make_async_copy(wu.at[0, e, r], buf.at[n, :, pl.ds(f, f)], lsem.at[n]).start()
            else:
                pltpu.make_async_copy(wd.at[0, e, r], buf.at[n], lsem.at[n]).start()

        @pl.when(own == 0)
        def _():
            pltpu.make_async_copy((r13 if wide else r2).at[j, r], (o13 if wide else o2).at[0, j, r], ssem.at[n]).start()

    for n, j, b, own, e in jobs:
        wide = b < nblk[0]
        r = pl.ds(b * b13, b13) if wide else pl.ds((b - nblk[0]) * b2, b2)

        @pl.when(own == 1)
        def _():
            pltpu.make_async_copy(buf.at[n], buf.at[n], lsem.at[n]).wait()
            pltpu.make_async_copy(buf.at[n], (o13 if wide else o2).at[0, j, r], ssem.at[n]).start()
    for n, j, b, own, e in jobs:
        pltpu.make_async_copy(buf.at[n], buf.at[n], ssem.at[n]).wait()


def solution(mesh):
    anyspec = pl.BlockSpec(memory_space=pl.ANY)
    smem = pl.BlockSpec(memory_space=pltpu.SMEM)

    def body(wg, wu, wd, place):
        _, nexp, d, f = wg.shape
        dt = wg.dtype
        ra, rb = d // UNITS, f // UNITS
        wmax = max(HUB[c][v] + FWD[c][ACROSS[v]] for c in range(2) for v in range(8))
        dma = pltpu.SemaphoreType.DMA

        def three(*lead):
            return [pltpu.VMEM((*lead, ra, f), dt), pltpu.VMEM((*lead, ra, f), dt), pltpu.VMEM((*lead, rb, d), dt)]

        r13, r2 = pl.pallas_call(
            _remote,
            out_shape=(pltpu.VMEM((2, d, 2 * f), dt), pltpu.VMEM((2, f, d), dt)),
            in_specs=[smem, anyspec, anyspec, anyspec],
            out_specs=(anyspec, anyspec),
            scratch_shapes=[
                *three(wmax, nexp), *three(nexp),
                pltpu.VMEM((nexp, ra, f), dt), pltpu.VMEM((nexp, rb, d), dt),
                *three(RING, MAXS), *three(DSTAGE), *three(ORING),
                dma((3, wmax)), dma((3, wmax)), dma((3, RING, MAXS)), dma((3, DSTAGE)), dma((3, ORING)),
                dma((3,)), dma((2, 3)), pltpu.SemaphoreType.REGULAR, pltpu.SemaphoreType.REGULAR, dma((3, wmax)),
                pltpu.SemaphoreType.REGULAR((4,)),
            ],
            compiler_params=pltpu.CompilerParams(has_side_effects=True, collective_id=0, vmem_limit_bytes=39 * 1024 * 1024),
            name="spread",
        )(place, wg, wu, wd)
        r13 = pltpu.with_memory_space_constraint(r13, pltpu.VMEM)
        r2 = pltpu.with_memory_space_constraint(r2, pltpu.VMEM)
        nblk = (8, 4)
        nbuf = 2 * sum(nblk)
        return pl.pallas_call(
            functools.partial(_local, nblk),
            out_shape=(jax.ShapeDtypeStruct((1, 2, d, 2 * f), dt), jax.ShapeDtypeStruct((1, 2, f, d), dt)),
            in_specs=[smem, anyspec, anyspec, anyspec, anyspec, anyspec],
            out_specs=(anyspec, anyspec),
            scratch_shapes=[pltpu.VMEM((nbuf, d // nblk[0], 2 * f), dt), dma((nbuf,)), dma((nbuf,))],
            compiler_params=pltpu.CompilerParams(vmem_limit_bytes=39 * 1024 * 1024),
            name="settle",
        )(place, wg, wu, wd, r13, r2)

    spec_in = P(None, "ep", None, None)
    spec_out = P(None, ("dp", "ep"), None, None)
    return jax.shard_map(body, mesh=mesh, in_specs=(spec_in, spec_in, spec_in, P(None, None)),
                         out_specs=(spec_out, spec_out), check_vma=False)
```

```python
import functools

import jax
import jax.numpy as jnp
from jax import lax
from jax.experimental import pallas as pl
from jax.experimental.pallas import tpu as pltpu
from jax.sharding import PartitionSpec as P

SUB = 1
UNITS = 32 * SUB
RING = 4 * SUB
ORING = 2
OWN = 8 * SUB
DSTAGE = 22 * SUB

def _rows(*digits):
    return tuple(tuple(SUB * int(d) for d in row) for row in digits)


HUB = _rows("56444405", "00666662")
FWD = _rows("00444400", "00000000")
THERE = (
    _rows("00000000", "00000000", "00004444", "00004434",
          "44440000", "44440000", "00000000", "00000000"),
    _rows(*[8 * "0"] * 8),
)
SERVE = (
    _rows("55532000", "66660600", "44440000", "44440000",
          "00004444", "00004444", "00000000", "00154555"),
    _rows("00000000", "00000000", "66666650", "46666600",
          "20666660", "04666660", "00606660", "00022220"),
)
KIND = []
for _a in range(8):
    _row = []
    for _c in range(2):
        for _j in range(2):
            _g = _c + 2
            _h = (2 * _a - _g) % 4 if _j < ((_a + 1) * 2) // 8 else (_g + _j + 1) % 4
            _row.append(_h if _h < 2 else (3 if _h == _g else 2))
    KIND.append(_row)
SLOTS = tuple(tuple((a, s // 2, s % 2) for a in range(8) for s in range(4) if KIND[a][s] == c) for c in range(2))
ACROSS = tuple(2 * (3 - v // 2) + v % 2 for v in range(8))
FIRST = tuple(tuple(sum(HUB[c][:v]) for v in range(8)) for c in range(2))


def _direct(c, u):
    if not any(s[0] == u for s in SLOTS[c]):
        return []
    out = []
    parts = [(FIRST[c][v] + THERE[c][v][u] + SERVE[c][v][u], FIRST[c][v] + HUB[c][v]) for v in range(8)]
    for lo, hi in parts + [(sum(HUB[c]), UNITS)]:
        if lo == hi:
            continue
        if out and out[-1][1] == lo:
            out[-1][1] = hi
        else:
            out.append([lo, hi])
    return out


BUSY = tuple(tuple([q for q, s in enumerate(SLOTS[c]) if SERVE[c][v][s[0]] or THERE[c][ACROSS[v]][s[0]]] for v in range(8)) for c in range(2))
MAXS = max(len(b) for c in range(2) for b in BUSY[c])
DIRECT = tuple(tuple(_direct(c, u) for u in range(8)) for c in range(2))
NDIR = tuple(tuple(sum(hi - lo for lo, hi in r) for r in DIRECT[c]) for c in range(2))


def _pick(table, i):
    r = jnp.int32(table[0])
    for k in range(1, len(table)):
        if table[k] != table[0]:
            r = lax.select(i == k, jnp.int32(table[k]), r)
    return r


def _remote(place, wg, wu, wd, r13, r2, raw_g, raw_u, raw_d, dw_g, dw_u, dw_d, wk13, wk2, hs_g, hs_u, hs_d,
            ds_g, ds_u, ds_d, os_g, os_u, os_d, raw_rx, raw_tx, h_tx, d_tx, o_tx, ld, rx, clear, head, f_tx, ready):
    a = lax.axis_index("dp")
    g = lax.axis_index("ep")
    x = lax.div(g, 2)
    core = lax.rem(g, 2)
    w, raw, dw = (wg, wu, wd), (raw_g, raw_u, raw_d), (dw_g, dw_u, dw_d)
    hs, ds, os_, wk = (hs_g, hs_u, hs_d), (ds_g, ds_u, ds_d), (os_g, os_u, os_d), (wk13, wk13, wk2)
    nexp, f = wg.shape[1], wg.shape[3]
    rows = tuple(r.shape[2] for r in raw)

    def expert(s, h):
        return jnp.clip(place[0, s] - h * nexp, 0, nexp - 1)

    def unit(t, k):
        return pl.ds(pl.multiple_of(k * rows[t], rows[t]), rows[t])

    def landing(t, j, k):
        if t == 2:
            return r2.at[j, unit(t, k)]
        return r13.at[j, unit(t, k), pl.ds(t * f, f)]

    def send(t, src, j, k, tx, ua, uep):
        return pltpu.make_async_remote_copy(
            src_ref=src, dst_ref=landing(t, j, k), send_sem=tx, recv_sem=rx.at[j, t],
            device_id={"dp": ua, "ep": uep}, device_id_type=pl.DeviceIdType.MESH)

    z, y = lax.div(a, 2), lax.rem(a, 2)

    def tell(sem, dp, ep):
        pl.semaphore_signal(sem, 1, device_id={"dp": dp, "ep": ep}, device_id_type=pl.DeviceIdType.MESH)

    def tell_z(sem):
        @pl.when(z > 0)
        def _():
            tell(sem, a - 2, g)

        @pl.when(z < 3)
        def _():
            tell(sem, a + 2, g)

    nz = _pick((1, 2, 2, 1), z)

    barrier = pltpu.get_barrier_semaphore()
    other = 2 * x + 1 - core
    tell(barrier, a, 2 - 2 * x)
    tell(barrier, a, 3 - 2 * x)
    tell(barrier, a, other)
    tell(barrier, 2 * z + 1 - y, g)
    tell_z(barrier)
    pl.semaphore_wait(barrier, 4 + nz)

    def meet():
        for r in range(2):
            tell_z(ready.at[r])
            pl.semaphore_wait(ready.at[r], nz)
        tell(ready.at[2], 2 * z + 1 - y, g)
        pl.semaphore_wait(ready.at[2], 1)
        tell(ready.at[3], a, other)
        pl.semaphore_wait(ready.at[3], 1)

    for c in range(2):

        @pl.when(core == c)
        def _(c=c):
            width = _pick(HUB[c], a)
            first = _pick(FIRST[c], a)
            slots = SLOTS[c]
            nfwd = _pick(FWD[c], a)
            across = _pick(ACROSS, a)
            nmore = _pick([FWD[c][ACROSS[v]] for v in range(8)], a)
            wacross = _pick([HUB[c][ACROSS[v]] for v in range(8)], a)
            shift = _pick([FIRST[c][ACROSS[v]] - HUB[c][v] for v in range(8)], a)
            low = [_pick([THERE[c][v][s[0]] for v in range(8)], a) for s in slots]
            high = [_pick([THERE[c][v][s[0]] + SERVE[c][v][s[0]] for v in range(8)], a) for s in slots]
            more = [_pick([HUB[c][v] + THERE[c][ACROSS[v]][s[0]] for v in range(8)], a) for s in slots]

            def hunit(i):
                return lax.select(i < width, first, shift) + i

            def forward(i, t):
                return pltpu.make_async_remote_copy(
                    src_ref=raw[t].at[i], dst_ref=raw[t].at[wacross + i], send_sem=f_tx.at[t, i],
                    recv_sem=raw_rx.at[t, wacross + i],
                    device_id={"dp": across, "ep": g}, device_id_type=pl.DeviceIdType.MESH)

            def raw_copy(i, t):
                return pltpu.make_async_remote_copy(
                    src_ref=w[t].at[0, :, unit(t, first + i)], dst_ref=raw[t].at[i],
                    send_sem=raw_tx.at[t, i], recv_sem=raw_rx.at[t, i],
                    device_id={"dp": a, "ep": 2 * (1 - x) + c}, device_id_type=pl.DeviceIdType.MESH)

            def raw_start(i, _):
                for t in range(3):
                    raw_copy(i, t).start()
                return _

            if c == 0:
                lax.fori_loop(0, width, raw_start, 0)
                meet()

                @pl.when(width > 0)
                def _():
                    raw_copy(0, 0).wait_send()

                tell(head, a, g + 1)
            else:
                meet()
                pl.semaphore_wait(head, 1)
                lax.fori_loop(0, width, raw_start, 0)

            dslots = [[(s[1], s[2]) for s in slots if s[0] == u] if NDIR[c][u] else [] for u in range(8)]
            per = max(len(s) for s in dslots)
            count = _pick([max(len(s), 1) for s in dslots], a)
            ndir = _pick(NDIR[c], a)
            nranges = max(len(r) for r in DIRECT[c])
            starts, steps = [], []
            base = _pick([r[0][0] if r else 0 for r in DIRECT[c]], a)
            for q in range(1, nranges):
                starts.append(_pick([sum(hi - lo for lo, hi in r[:q]) if len(r) > q else 999 for r in DIRECT[c]], a))
                steps.append(_pick([r[q][0] - r[q - 1][1] if len(r) > q else 0 for r in DIRECT[c]], a))

            nown = _pick([UNITS if 2 in KIND[u][:2] else 0 for u in range(8)], a) if c == 1 else jnp.int32(0)
            njobs = nown + ndir

            def dunit(n):
                k = base + n
                for st, sp in zip(starts, steps):
                    k = k + lax.select(n >= st, sp, jnp.int32(0))
                return k

            def junit(n):
                return lax.select(n < nown, n, dunit(n - nown)) if c == 1 else dunit(n)

            def load(n, t):
                return pltpu.make_async_copy(w[t].at[0, :, unit(t, junit(n))], dw[t], ld.at[t])

            dtab = []
            for q in range(per):
                dtab.append((_pick([len(s) > q for s in dslots], a),
                             _pick([s[q][0] if len(s) > q else 0 for s in dslots], a),
                             _pick([s[q][1] if len(s) > q else 0 for s in dslots], a)))
                dtab[q] += (expert((a * 4 + 2 * (1 - x) + dtab[q][1]) * 2 + dtab[q][2], 2 * x + c),)
            eown = expert((a * 4 + 2 * x) * 2, 2 * x + c)

            def dsend(n, t, q):
                _, uc, j, _ = dtab[q]
                return send(t, ds[t].at[n * count + q], j, dunit(n), d_tx.at[t, n * count + q], a, 2 * (1 - x) + uc)

            def osend(n, t):
                return send(t, os_[t].at[lax.rem(n, ORING)], 0, n, o_tx.at[t, lax.rem(n, ORING)], a, 2 * x)

            @pl.when(njobs > 0)
            def _():
                for t in range(3):
                    load(0, t).start()

            def direct(n):
                for t in range(3):
                    load(n, t).wait()
                    wk[t][...] = dw[t][...]

                    @pl.when(n + 1 < njobs)
                    def _():
                        load(n + 1, t).start()

                    @pl.when(n >= nown)
                    def _():
                        m = n - nown
                        for q in range(per):
                            @pl.when(dtab[q][0] == 1)
                            def _():
                                e = dtab[q][3]
                                ds[t][m * count + q] = wk[t][e]

                        for q in range(per):

                            @pl.when(dtab[q][0] == 1)
                            def _():
                                dsend(m, t, q).start()

                    if c == 1:

                        @pl.when(n < nown)
                        def _():
                            @pl.when(n >= ORING)
                            def _():
                                osend(n - ORING, t).wait_send()

                            os_[t][lax.rem(n, ORING)] = wk[t][eown]
                            osend(n, t).start()

            picks = [expert((ua * 4 + 2 * x + uc) * 2 + j, 2 * (1 - x) + c) for ua, uc, j in slots]

            spot = [_pick([b.index(q) if q in b else 0 for b in BUSY[c]], a) for q in range(len(slots))]

            def serving(i):
                mine = i < width
                zero = jnp.int32(0)
                return [(i >= lax.select(mine, low[q], zero)) & (i < lax.select(mine, high[q], more[q]))
                        for q in range(len(slots))]

            def hub_do(p, k, t, q, start):
                ua, uc, j = slots[q]
                src, tx = hs[t].at[p, spot[q]], h_tx.at[t, p, spot[q]]

                def far():
                    cp = send(t, src, j, k, tx, ua, 2 * x + uc)
                    cp.start() if start else cp.wait_send()

                if uc != c:
                    far()
                    return
                pl.when(a != ua)(far)

                @pl.when(a == ua)
                def _():
                    cp = pltpu.make_async_copy(src, landing(t, j, k), tx)
                    cp.start() if start else cp.wait()

            def hub_free(i, on, p, t):
                k = hunit(i)
                for q in range(len(slots)):
                    pl.when(on[q])(functools.partial(hub_do, p, k, t, q, False))

            def hub(i):
                p = lax.rem(i, RING)
                k = hunit(i)
                on = serving(i)
                for t in range(3):

                    @pl.when(i >= RING)
                    def _():
                        hub_free(i - RING, serving(i - RING), p, t)

                    pltpu.make_async_copy(raw[t].at[i], raw[t].at[i], raw_rx.at[t, i]).wait()

                    @pl.when(i < nfwd)
                    def _():
                        forward(i, t).start()

                    wk[t][...] = raw[t][i]
                    for q in range(len(slots)):

                        @pl.when(on[q])
                        def _():
                            hs[t][p, spot[q]] = wk[t][picks[q]]

                    for q in range(len(slots)):
                        pl.when(on[q])(functools.partial(hub_do, p, k, t, q, True))

            def loop(lo, hi, f):
                lax.fori_loop(lo, hi, lambda i, s: (f(i), s)[1], 0)

            def raw_drain(i):
                for t in range(3):
                    if c == 0 and t == 0:

                        @pl.when(i > 0)
                        def _():
                            raw_copy(i, 0).wait_send()
                    else:
                        raw_copy(i, t).wait_send()

            most = jnp.maximum(width - 1, 0)
            early = _pick((0, 0, 1, 1, 1, 1, 0, 0), a)

            def drain_most(i):
                @pl.when(i < most)
                def _():
                    raw_drain(i)

            def direct_some(n):
                @pl.when(n < njobs)
                def _():
                    direct(n)

            def mixed(i):
                @pl.when(i == most)
                def _():
                    loop(0, max(HUB[c]) - 1, drain_most)
                    pl.semaphore_signal(clear, 1, device_id={"dp": a, "ep": 2 * x + 1 - c},
                                        device_id_type=pl.DeviceIdType.MESH)
                    if c == 0:

                        @pl.when(early == 1)
                        def _():
                            loop(0, max(NDIR[0]), direct_some)

                def pair(r):
                    @pl.when(i < lax.select(r == 0, width, nmore))
                    def _():
                        hub(i + r * width)

                loop(0, 2, pair)
                if c == 1:

                    @pl.when(i * OWN < nown)
                    def _():
                        loop(0, OWN, lambda r: direct(i * OWN + r))

            ntimes = [max(HUB[c][v], FWD[c][ACROSS[v]], UNITS // OWN if c == 1 and 2 in KIND[v][:2] else 1) for v in range(8)]
            loop(0, _pick(ntimes, a), mixed)

            if c == 0:

                @pl.when(early == 0)
                def _():
                    pl.semaphore_wait(clear, 1)
                    loop(nown, njobs, direct)

                @pl.when(early == 1)
                def _():
                    pl.semaphore_wait(clear, 1)
            else:
                pl.semaphore_wait(clear, 1)
                loop(nown, njobs, direct)
            loop(most, width, raw_drain)

            def forward_drain(i):
                for t in range(3):
                    forward(i, t).wait_send()

            loop(0, nfwd, forward_drain)

            def hub_drain(i, s):
                on = serving(i)
                for t in range(3):
                    hub_free(i, on, lax.rem(i, RING), t)
                return s

            lax.fori_loop(jnp.maximum(width + nmore - RING, 0), width + nmore, hub_drain, 0)

            def direct_drain(n, s):
                for t in range(3):
                    for q in range(per):

                        @pl.when(dtab[q][0] == 1)
                        def _():
                            dsend(n, t, q).wait_send()
                return s

            lax.fori_loop(0, ndir, direct_drain, 0)
            if c == 1:

                def own_drain(n, s):
                    for t in range(3):
                        osend(n, t).wait_send()
                    return s

                lax.fori_loop(jnp.maximum(nown - ORING, 0), nown, own_drain, 0)

            for u in range(8):

                @pl.when(a == u)
                def _(u=u):
                    for j in range(2):
                        kind = KIND[u][2 * c + j]
                        if kind == 3:
                            continue
                        n = UNITS - (SERVE[c][u][u] + THERE[c][ACROSS[u]][u] if kind == c else 0)
                        for t in range(3):
                            if t == 2:
                                part = r2.at[j, pl.ds(0, n * rows[2])]
                            else:
                                part = r13.at[j, pl.ds(0, n * rows[t]), pl.ds(t * f, f)]
                            pltpu.make_async_copy(part, part, rx.at[j, t]).wait()


def _local(nblk, place, wg, wu, wd, r13, r2, o13, o2, buf, lsem, ssem):
    a = lax.axis_index("dp")
    g = lax.axis_index("ep")
    nexp, f = wg.shape[1], wg.shape[3]
    b13 = r13.shape[1] // nblk[0]
    b2 = r2.shape[1] // nblk[1]
    n = 0
    jobs = []
    for j in range(2):
        own = jnp.int32(0)
        for u in range(8):
            for c in range(2):
                if KIND[u][2 * c + j] == 3:
                    own = jnp.where((a == u) & (g % 2 == c), 1, own)
        e = jnp.clip(place[0, (a * 4 + g) * 2 + j] - g * nexp, 0, nexp - 1)
        for b in range(nblk[0] + nblk[1]):
            jobs.append((n, j, b, own, e))
            n += 1
    for n, j, b, own, e in jobs:
        wide = b < nblk[0]
        r = pl.ds(b * b13, b13) if wide else pl.ds((b - nblk[0]) * b2, b2)

        @pl.when(own == 1)
        def _():
            if wide:
                pltpu.make_async_copy(wg.at[0, e, r], buf.at[n, :, pl.ds(0, f)], lsem.at[n]).start()
                pltpu.make_async_copy(wu.at[0, e, r], buf.at[n, :, pl.ds(f, f)], lsem.at[n]).start()
            else:
                pltpu.make_async_copy(wd.at[0, e, r], buf.at[n], lsem.at[n]).start()

        @pl.when(own == 0)
        def _():
            pltpu.make_async_copy((r13 if wide else r2).at[j, r], (o13 if wide else o2).at[0, j, r], ssem.at[n]).start()

    for n, j, b, own, e in jobs:
        wide = b < nblk[0]
        r = pl.ds(b * b13, b13) if wide else pl.ds((b - nblk[0]) * b2, b2)

        @pl.when(own == 1)
        def _():
            pltpu.make_async_copy(buf.at[n], buf.at[n], lsem.at[n]).wait()
            pltpu.make_async_copy(buf.at[n], (o13 if wide else o2).at[0, j, r], ssem.at[n]).start()
    for n, j, b, own, e in jobs:
        pltpu.make_async_copy(buf.at[n], buf.at[n], ssem.at[n]).wait()


def solution(mesh):
    anyspec = pl.BlockSpec(memory_space=pl.ANY)
    smem = pl.BlockSpec(memory_space=pltpu.SMEM)

    def body(wg, wu, wd, place):
        _, nexp, d, f = wg.shape
        dt = wg.dtype
        ra, rb = d // UNITS, f // UNITS
        wmax = max(HUB[c][v] + FWD[c][ACROSS[v]] for c in range(2) for v in range(8))
        dma = pltpu.SemaphoreType.DMA

        def three(*lead):
            return [pltpu.VMEM((*lead, ra, f), dt), pltpu.VMEM((*lead, ra, f), dt), pltpu.VMEM((*lead, rb, d), dt)]

        r13, r2 = pl.pallas_call(
            _remote,
            out_shape=(pltpu.VMEM((2, d, 2 * f), dt), pltpu.VMEM((2, f, d), dt)),
            in_specs=[smem, anyspec, anyspec, anyspec],
            out_specs=(anyspec, anyspec),
            scratch_shapes=[
                *three(wmax, nexp), *three(nexp),
                pltpu.VMEM((nexp, ra, f), dt), pltpu.VMEM((nexp, rb, d), dt),
                *three(RING, MAXS), *three(DSTAGE), *three(ORING),
                dma((3, wmax)), dma((3, wmax)), dma((3, RING, MAXS)), dma((3, DSTAGE)), dma((3, ORING)),
                dma((3,)), dma((2, 3)), pltpu.SemaphoreType.REGULAR, pltpu.SemaphoreType.REGULAR, dma((3, wmax)),
                pltpu.SemaphoreType.REGULAR((4,)),
            ],
            compiler_params=pltpu.CompilerParams(has_side_effects=True, collective_id=0, vmem_limit_bytes=39 * 1024 * 1024),
            name="spread",
        )(place, wg, wu, wd)
        r13 = pltpu.with_memory_space_constraint(r13, pltpu.VMEM)
        r2 = pltpu.with_memory_space_constraint(r2, pltpu.VMEM)
        nblk = (16, 8)
        nbuf = 2 * sum(nblk)
        return pl.pallas_call(
            functools.partial(_local, nblk),
            out_shape=(jax.ShapeDtypeStruct((1, 2, d, 2 * f), dt), jax.ShapeDtypeStruct((1, 2, f, d), dt)),
            in_specs=[smem, anyspec, anyspec, anyspec, anyspec, anyspec],
            out_specs=(anyspec, anyspec),
            scratch_shapes=[pltpu.VMEM((nbuf, d // nblk[0], 2 * f), dt), dma((nbuf,)), dma((nbuf,))],
            compiler_params=pltpu.CompilerParams(vmem_limit_bytes=39 * 1024 * 1024),
            name="settle",
        )(place, wg, wu, wd, r13, r2)

    spec_in = P(None, "ep", None, None)
    spec_out = P(None, ("dp", "ep"), None, None)
    return jax.shard_map(body, mesh=mesh, in_specs=(spec_in, spec_in, spec_in, P(None, None)),
                         out_specs=(spec_out, spec_out), check_vma=False)
```
